8 devices in a mesh: dp: 1 (over z), tp: 2 (over y), cp: 4 (over x, core).
Axes of the slice: x: 2, y: 2, z: 1, core: 2. Of those that a mesh axis runs over, the one named last changes fastest.
Arguments:
- x: bfloat16 [2048, 3072], P(('dp', 'cp'))
- doc_ids: int32 [2048], P(('dp', 'cp'))
- w_query: bfloat16 [3072, 3072], P(None, 'tp')
- w_key: bfloat16 [3072, 1024], P(None, 'tp')
- w_value: bfloat16 [3072, 1024], P(None, 'tp')
- w_out: bfloat16 [3072, 3072], P('tp')
Outputs:
- output: bfloat16 [2048, 3072], P(('dp', 'cp'))
All inputs are finite; a program needn't handle non-finite values.
Results may differ from the reference program's by a relative error of at most 0.00727143.
Values are sent between devices in bfloat16 or wider.
A program may use at most 1 GiB of HBM per device.

```python
import jax
import jax.numpy as jnp
from jax import lax

SEQ_LEN = 2048
BLOCK_LEN = 256
DOC_BREAKS = 16
D = 3072
HEADS = 24
KV_HEADS = 8
HEAD = 128


def setup_inputs(seed: int = 0, part: int = 0) -> dict:
    shared_keys = jax.random.split(jax.random.key(seed), 4)
    part_keys = jax.random.split(jax.random.fold_in(jax.random.key(seed + 1), part), 4)
    x = jax.random.normal(part_keys[0], (SEQ_LEN, D), jnp.float32).astype(jnp.bfloat16)
    span_len = jax.random.randint(part_keys[1], (), SEQ_LEN // 3, 2 * SEQ_LEN // 3 + 1)
    span_start = jax.random.randint(part_keys[2], (), 0, SEQ_LEN - span_len + 1)
    breaks = jax.random.randint(part_keys[3], (DOC_BREAKS,), 1, SEQ_LEN)
    inside = (breaks > span_start) & (breaks < span_start + span_len)
    start_flags = jnp.zeros((SEQ_LEN,), jnp.int32).at[breaks].add(jnp.where(inside, 0, 1))
    doc_ids = jnp.cumsum(start_flags).astype(jnp.int32)
    w_query = (jax.random.normal(shared_keys[0], (D, HEADS * HEAD), jnp.float32) * (1.5 / D ** 0.5)).astype(jnp.bfloat16)
    w_key = (jax.random.normal(shared_keys[1], (D, KV_HEADS * HEAD), jnp.float32) * (1.5 / D ** 0.5)).astype(jnp.bfloat16)
    w_value = (jax.random.normal(shared_keys[2], (D, KV_HEADS * HEAD), jnp.float32) / D ** 0.5).astype(jnp.bfloat16)
    w_out = (jax.random.normal(shared_keys[3], (HEADS * HEAD, D), jnp.float32) * (2.0 / (HEADS * HEAD) ** 0.5)).astype(jnp.bfloat16)
    return {'x': x, 'doc_ids': doc_ids, 'w_query': w_query, 'w_key': w_key, 'w_value': w_value, 'w_out': w_out}


def block_update(soft_state, q_blk, k_blk, v_blk, allowed):
    run_max, run_sum, out_acc = soft_state
    scores = jnp.einsum('qhgd,khd->qhgk', q_blk.astype(jnp.float32), k_blk.astype(jnp.float32)) * (HEAD ** -0.5)
    scores = jnp.where(allowed[:, None, None, :], scores, -jnp.inf)
    new_max = jnp.maximum(run_max, jnp.max(scores, axis=-1))
    safe_max = jnp.where(new_max == -jnp.inf, 0.0, new_max)
    prob_vals = jnp.exp(scores - safe_max[..., None])
    rescale = jnp.exp(run_max - safe_max)
    run_sum = run_sum * rescale + jnp.sum(prob_vals, axis=-1)
    out_acc = out_acc * rescale[..., None] + jnp.einsum('qhgk,khd->qhgd', prob_vals, v_blk.astype(jnp.float32))
    return new_max, run_sum, out_acc


def reference(x, doc_ids, w_query, w_key, w_value, w_out):
    q_per_kv = HEADS // KV_HEADS
    n_blocks = SEQ_LEN // BLOCK_LEN
    q_all = jnp.dot(x, w_query, preferred_element_type=jnp.float32).astype(jnp.bfloat16).reshape(n_blocks, BLOCK_LEN, KV_HEADS, q_per_kv, HEAD)
    k_all = jnp.dot(x, w_key, preferred_element_type=jnp.float32).astype(jnp.bfloat16).reshape(n_blocks, BLOCK_LEN, KV_HEADS, HEAD)
    v_all = jnp.dot(x, w_value, preferred_element_type=jnp.float32).astype(jnp.bfloat16).reshape(n_blocks, BLOCK_LEN, KV_HEADS, HEAD)
    seg_blocks = doc_ids.reshape(n_blocks, BLOCK_LEN)
    pos_blocks = jnp.arange(SEQ_LEN).reshape(n_blocks, BLOCK_LEN)

    def query_block(q_inputs):
        q_blk, seg_q, pos_q = q_inputs

        def key_step(soft_state, k_inputs):
            k_blk, v_blk, seg_k, pos_k = k_inputs
            active = (pos_k[0] <= pos_q[BLOCK_LEN - 1]) & (seg_k[BLOCK_LEN - 1] >= seg_q[0])
            allowed = (seg_q[:, None] == seg_k[None, :]) & (pos_q[:, None] >= pos_k[None, :])
            new_state = lax.cond(active, lambda same_state: block_update(same_state, q_blk, k_blk, v_blk, allowed), lambda same_state: same_state, soft_state)
            return new_state, None

        init_state = (jnp.full((BLOCK_LEN, KV_HEADS, q_per_kv), -jnp.inf, jnp.float32), jnp.zeros((BLOCK_LEN, KV_HEADS, q_per_kv), jnp.float32), jnp.zeros((BLOCK_LEN, KV_HEADS, q_per_kv, HEAD), jnp.float32))
        final_state = lax.scan(key_step, init_state, (k_all, v_all, seg_blocks, pos_blocks))[0]
        run_sum = final_state[1]
        out_acc = final_state[2]
        return (out_acc / run_sum[..., None]).astype(jnp.bfloat16).reshape(BLOCK_LEN, HEADS * HEAD)

    heads_out = lax.map(query_block, (q_all, seg_blocks, pos_blocks)).reshape(SEQ_LEN, HEADS * HEAD)
    return jnp.dot(heads_out, w_out, preferred_element_type=jnp.float32).astype(jnp.bfloat16)
```

```python
import math

import jax
import jax.numpy as jnp
from jax import lax
from jax.experimental import pallas as pl
from jax.experimental.pallas import tpu as pltpu
from jax.sharding import PartitionSpec as P

HEAD = 128
TILE = 256
COLS = 512
MESH = pl.DeviceIdType.MESH
F32 = jnp.float32
BF16 = jnp.bfloat16
SCALE = HEAD ** -0.5 * math.log2(math.e)


def layer_kernel(seg_hbm, x_hbm, wq_hbm, wk_hbm, wv_hbm, wo_hbm, y_hbm,
                 seg, segq, xbuf, wbuf, kv, q, o_own, o_oth, wo, w_oth, y_own, y_oth,
                 load_sem, tile_sem, out_sem, seg_s, seg_r, kv_s, kv_r,
                 y_s, y_r, xf_s, xf_r, d1_s, d1_r, d2_s, d2_r, o_s, o_r):
    chunk, width = xbuf.shape
    kv_heads = kv.shape[0] // 2
    heads = q.shape[0]
    group = heads // kv_heads
    n_blocks = seg.shape[0]
    quarter = wo.shape[0] // n_blocks
    pieces = y_s.shape[0]
    piece = quarter // pieces
    n_cols = width // COLS
    kv_tiles = 2 * kv_heads * HEAD // TILE
    q_tiles = heads * HEAD // TILE
    slots = wbuf.shape[0]

    dp = lax.axis_index('dp')
    tp = lax.axis_index('tp')
    me = lax.axis_index('cp')
    core_peer = me + 1 - 2 * lax.rem(me, 2)
    chip_peer = lax.rem(me + 2, 4)
    far_peer = 3 - me
    tp_peer = (dp, 1 - tp, me)

    def at(block):
        return (dp, tp, block)

    def remote(src, dst, s_sem, r_sem, where):
        return pltpu.make_async_remote_copy(src_ref=src, dst_ref=dst, send_sem=s_sem, recv_sem=r_sem,
                                            device_id=where, device_id_type=MESH)

    def kv_tile_src(t):
        per = kv_tiles // 2
        return (wk_hbm if t < per else wv_hbm).at[:, pl.ds((t % per) * TILE, TILE)]

    def tile_copy(src, slot):
        return pltpu.make_async_copy(src, wbuf.at[slot], tile_sem.at[slot])

    def q_tile_src(t):
        return wq_hbm.at[:, pl.ds(pl.multiple_of(t * TILE, TILE), TILE)]

    x_load = pltpu.make_async_copy(x_hbm, xbuf, load_sem.at[0])
    wo_load = pltpu.make_async_copy(wo_hbm, wo, load_sem.at[1])
    seg_load = pltpu.make_async_copy(seg_hbm, seg.at[me], load_sem.at[2])
    x_load.start()
    for t in range(kv_tiles):
        tile_copy(kv_tile_src(t), t).start()
    seg_load.start()

    barrier = pltpu.get_barrier_semaphore()
    for where in (tp_peer, at(core_peer), at(chip_peer), at(far_peer)):
        pl.semaphore_signal(barrier, inc=1, device_id=where, device_id_type=MESH)
    pl.semaphore_wait(barrier, 4)

    def rows_of(block, i):
        return pl.ds(pl.multiple_of(block * quarter + i * piece, piece), piece)

    def y_copy(i):
        return remote(wo_hbm.at[rows_of(me, i)], w_oth.at[rows_of(me, i)], y_s.at[i], y_r.at[i], tp_peer)

    def hand_on(block, i, s_sem, r_sem, where):
        part = w_oth.at[rows_of(block, i)]
        return remote(part, part, s_sem.at[i], r_sem.at[i], where)

    def seg_copy(k, block, where):
        return remote(seg.at[block], seg.at[block], seg_s.at[k], seg_r.at[k], where)

    def kv_copy(k, block, where):
        part = kv.at[:, pl.ds(pl.multiple_of(block * chunk, chunk), chunk), :]
        return remote(part, part, kv_s.at[k], kv_r.at[k], where)

    def o_copy(u):
        h = head_of(u)
        return remote(o_own.at[h], o_oth.at[h], o_s.at[u], o_r.at[u], tp_peer)

    def group_of(j):
        high = lax.rem(me // 2 + j // 2, 2)
        low = lax.rem(lax.rem(me, 2) + lax.rem(j, 2), 2)
        return 2 * high + low

    def head_of(u):
        return group_of(u // group) * group + lax.rem(u, group)

    for i in range(pieces):
        y_copy(i).start()
    seg_load.wait()
    for k, block in enumerate((core_peer, chip_peer, far_peer)):
        seg_copy(k, me, at(block)).start()

    x_load.wait()
    own_rows = pl.ds(pl.multiple_of(me * chunk, chunk), chunk)

    def project_kv(t, _):
        tile_copy(wk_hbm.at[:, pl.ds(0, TILE)], t).wait()
        part = jnp.dot(xbuf[...], wbuf[t], preferred_element_type=F32).astype(BF16)
        for k in range(TILE // HEAD):
            kv[t * (TILE // HEAD) + k, own_rows, :] = part[:, k * HEAD:(k + 1) * HEAD]

        @pl.when(t < q_tiles)
        def _():
            tile_copy(q_tile_src(t), t).start()
        return 0

    lax.fori_loop(0, kv_tiles, project_kv, 0)

    def project_q(t, _):
        slot = lax.rem(t, slots)
        tile_copy(q_tile_src(t), slot).wait()
        part = jnp.dot(xbuf[...], wbuf[slot], preferred_element_type=F32).astype(BF16)
        for k in range(TILE // HEAD):
            q[t * (TILE // HEAD) + k] = part[:, k * HEAD:(k + 1) * HEAD]

        @pl.when(t + slots < q_tiles)
        def _():
            tile_copy(q_tile_src(t + slots), slot).start()

        @pl.when(t == 0)
        def _():
            @pl.when(me < 2)
            def _():
                kv_copy(0, me, at(chip_peer)).start()
            kv_copy(1, me, at(core_peer)).start()
            wo_load.start()
        return 0

    lax.fori_loop(0, q_tiles, project_q, 0)

    def pass_y(i):
        y_copy(i).wait_recv()
        hand_on(me, i, xf_s, xf_r, at(chip_peer)).start()
        hand_on(me, i, d1_s, d1_r, at(core_peer)).start()

    def pass_x(i):
        hand_on(chip_peer, i, xf_s, xf_r, at(chip_peer)).wait_recv()
        hand_on(chip_peer, i, d2_s, d2_r, at(core_peer)).start()

    pass_y(0)
    for k, block in enumerate((core_peer, chip_peer, far_peer)):
        seg_copy(k, block, at(block)).wait_recv()
    seg_col = jnp.transpose(jnp.broadcast_to(seg[me], (HEAD, chunk)))
    segq[...] = seg_col

    kv_copy(1, core_peer, at(core_peer)).wait_recv()

    @pl.when(me >= 2)
    def _():
        kv_copy(0, chip_peer, at(chip_peer)).wait_recv()
        kv_copy(2, chip_peer, at(core_peer)).start()
        kv_copy(2, far_peer, at(core_peer)).wait_recv()

    def attend(h, g, r, n):
        rows = pl.ds(pl.multiple_of(r * TILE, TILE), TILE)
        q_t = q[h, rows, :]
        sq = segq[rows, :]
        sq = jnp.concatenate([sq] * (chunk // HEAD), axis=1)
        parts = []
        for b in range(n):
            s = lax.dot_general(q_t, kv[g, pl.ds(b * chunk, chunk), :], (((1,), (1,)), ((), ())), preferred_element_type=F32)
            ok = sq == seg[b]
            if b == n - 1:
                q_pos = r * TILE + lax.broadcasted_iota(jnp.int32, (TILE, chunk), 0)
                ok = ok & (q_pos >= lax.broadcasted_iota(jnp.int32, (TILE, chunk), 1))
            parts.append(jnp.where(ok, s, -jnp.inf))
        top = parts[0].max(axis=1, keepdims=True)
        for s in parts[1:]:
            top = jnp.maximum(top, s.max(axis=1, keepdims=True))
        total = None
        acc = None
        for b, s in enumerate(parts):
            p = jnp.exp2((s - top) * SCALE)
            row_sum = p.sum(axis=1, keepdims=True)
            pv = jnp.dot(p.astype(BF16), kv[kv_heads + g, pl.ds(b * chunk, chunk), :], preferred_element_type=F32)
            total = row_sum if total is None else total + row_sum
            acc = pv if acc is None else acc + pv
        o_own[h, rows, :] = (acc / total).astype(BF16)

    def attend_head(u, _):
        g = group_of(u // group)
        h = head_of(u)
        for n in range(1, n_blocks + 1):
            @pl.when(me == n - 1)
            def _(n=n):
                def one(r, c):
                    attend(h, g, r, n)
                    return c
                lax.fori_loop(0, chunk // TILE, one, 0)

        @pl.when(u > 0)
        def _():
            o_copy(u - 1).start()

        @pl.when(u == group - 1)
        def _():
            pass_y(1)

        @pl.when(u == 3 * group - 1)
        def _():
            pass_x(0)
        return 0

    lax.fori_loop(0, heads, attend_head, 0)
    pass_y(2)

    def add_rows(o_ref, w_ref, y_ref, h0, count, first):
        rows = pl.ds(pl.multiple_of(h0 * HEAD, HEAD), count * HEAD)

        def one(c, carry):
            cols = pl.ds(pl.multiple_of(c * COLS, COLS), COLS)
            left = jnp.concatenate([o_ref[h0 + k] for k in range(count)], axis=1)
            part = jnp.dot(left, w_ref[rows, cols], preferred_element_type=F32)
            y_ref[:, cols] = part if first else y_ref[:, cols] + part
            return carry

        lax.fori_loop(0, n_cols, one, 0)

    wo_load.wait()
    add_rows(o_own, wo, y_own, group_of(0) * group, group, True)
    o_copy(heads - 1).start()
    for j in range(1, kv_heads - 1):
        add_rows(o_own, wo, y_own, group_of(j) * group, group, False)
    last = group_of(kv_heads - 1) * group
    add_rows(o_own, wo, y_own, last, group - 1, False)
    add_rows(o_own, wo, y_own, last + group - 1, 1, False)

    pass_x(1)
    for u in range(group):
        o_copy(u).wait_recv()
    add_rows(o_oth, w_oth, y_oth, group_of(0) * group, group, True)
    for i in range(pieces):
        hand_on(core_peer, i, d1_s, d1_r, at(core_peer)).wait_recv()
    for u in range(group, 2 * group):
        o_copy(u).wait_recv()
    add_rows(o_oth, w_oth, y_oth, group_of(1) * group, group, False)
    pass_x(2)
    for u in range(2 * group, 3 * group):
        o_copy(u).wait_recv()
    add_rows(o_oth, w_oth, y_oth, group_of(2) * group, group, False)
    for i in range(pieces):
        hand_on(far_peer, i, d2_s, d2_r, at(core_peer)).wait_recv()
    for u in range(3 * group, heads - 1):
        o_copy(u).wait_recv()
    add_rows(o_oth, w_oth, y_oth, last, group - 1, False)
    o_copy(heads - 1).wait_recv()

    def out_copy(c):
        cols = pl.ds(pl.multiple_of(c * COLS, COLS), COLS)
        return pltpu.make_async_copy(xbuf.at[:, cols], y_hbm.at[:, cols], out_sem.at[c])

    def finish(c, carry):
        h = last + group - 1
        cols = pl.ds(pl.multiple_of(c * COLS, COLS), COLS)
        part = jnp.dot(o_oth[h], w_oth[pl.ds(pl.multiple_of(h * HEAD, HEAD), HEAD), cols], preferred_element_type=F32)
        xbuf[:, cols] = (y_own[:, cols] + (y_oth[:, cols] + part)).astype(BF16)
        out_copy(c).start()
        return carry

    lax.fori_loop(0, n_cols, finish, 0)

    for i in range(pieces):
        y_copy(i).wait_send()
        hand_on(me, i, xf_s, xf_r, at(chip_peer)).wait_send()
        hand_on(me, i, d1_s, d1_r, at(core_peer)).wait_send()
        hand_on(chip_peer, i, d2_s, d2_r, at(core_peer)).wait_send()
    for k, block in enumerate((core_peer, chip_peer, far_peer)):
        seg_copy(k, me, at(block)).wait_send()
    kv_copy(1, me, at(core_peer)).wait_send()

    @pl.when(me < 2)
    def _():
        kv_copy(0, me, at(chip_peer)).wait_send()

    @pl.when(me >= 2)
    def _():
        kv_copy(2, chip_peer, at(core_peer)).wait_send()

    for u in range(heads):
        o_copy(u).wait_send()
    for c in range(n_cols):
        out_copy(c).wait()


def solution(mesh):
    n_blocks = mesh.shape['cp']

    def layer(x_loc, seg_loc, w_query, w_key, w_value, w_out):
        chunk, width = x_loc.shape
        kv_heads = w_key.shape[1] // HEAD
        heads = w_query.shape[1] // HEAD
        pieces = 3
        dma = pltpu.SemaphoreType.DMA
        any_spec = pl.BlockSpec(memory_space=pl.ANY)
        return pl.pallas_call(
            layer_kernel,
            out_shape=jax.ShapeDtypeStruct((chunk, width), BF16),
            in_specs=[any_spec] * 6,
            out_specs=any_spec,
            scratch_shapes=[
                pltpu.VMEM((n_blocks, 1, chunk), jnp.int32),
                pltpu.VMEM((chunk, HEAD), jnp.int32),
                pltpu.VMEM((chunk, width), BF16),
                pltpu.VMEM((4, width, TILE), BF16),
                pltpu.VMEM((2 * kv_heads, n_blocks * chunk, HEAD), BF16),
                pltpu.VMEM((heads, chunk, HEAD), BF16),
                pltpu.VMEM((heads, chunk, HEAD), BF16),
                pltpu.VMEM((heads, chunk, HEAD), BF16),
                pltpu.VMEM(w_out.shape, BF16),
                pltpu.VMEM(w_out.shape, BF16),
                pltpu.VMEM((chunk, width), F32),
                pltpu.VMEM((chunk, width), F32),
                dma((3,)), dma((4,)), dma((width // COLS,)),
                dma((3,)), dma((3,)), dma((3,)), dma((3,)),
                dma((pieces,)), dma((pieces,)), dma((pieces,)), dma((pieces,)),
                dma((pieces,)), dma((pieces,)), dma((pieces,)), dma((pieces,)),
                dma((heads,)), dma((heads,)),
            ],
            compiler_params=pltpu.CompilerParams(collective_id=0, has_side_effects=True, vmem_limit_bytes=67043328),
        )(seg_loc.reshape(1, chunk), x_loc, w_query, w_key, w_value, w_out)

    rows = P(('dp', 'cp'), None)
    return jax.shard_map(layer, mesh=mesh,
                         in_specs=(rows, P(('dp', 'cp')), P(None, 'tp'), P(None, 'tp'), P(None, 'tp'), P('tp', None)),
                         out_specs=rows, check_vma=False)
```

```python
import math

import jax
import jax.numpy as jnp
from jax import lax
from jax.experimental import pallas as pl
from jax.experimental.pallas import tpu as pltpu
from jax.sharding import PartitionSpec as P

HEAD = 128
TILE = 256
COLS = 512
MESH = pl.DeviceIdType.MESH
F32 = jnp.float32
BF16 = jnp.bfloat16
SCALE = HEAD ** -0.5 * math.log2(math.e)


def layer_kernel(seg_hbm, x_hbm, wq_hbm, wk_hbm, wv_hbm, wo_hbm, y_out,
                 seg, segq, xbuf, wbuf, kv, q, o_own, o_oth, wo, w_oth, y_own, y_oth,
                 load_sem, tile_sem, seg_s, seg_r, kv_s, kv_r,
                 y_s, y_r, xf_s, xf_r, d1_s, d1_r, d2_s, d2_r, o_s, o_r):
    chunk, width = xbuf.shape
    kv_heads = kv.shape[0] // 2
    heads = q.shape[0]
    group = heads // kv_heads
    n_blocks = seg.shape[0]
    quarter = wo.shape[0] // n_blocks
    pieces = y_s.shape[0]
    piece = quarter // pieces
    n_cols = width // COLS
    kv_tiles = 2 * kv_heads * HEAD // TILE
    q_tiles = heads * HEAD // TILE
    slots = wbuf.shape[0]
    ends = chunk // HEAD

    dp = lax.axis_index('dp')
    tp = lax.axis_index('tp')
    me = lax.axis_index('cp')
    core_peer = me + 1 - 2 * lax.rem(me, 2)
    chip_peer = lax.rem(me + 2, 4)
    far_peer = 3 - me
    tp_peer = (dp, 1 - tp, me)

    def at(block):
        return (dp, tp, block)

    def remote(src, dst, s_sem, r_sem, where):
        return pltpu.make_async_remote_copy(src_ref=src, dst_ref=dst, send_sem=s_sem, recv_sem=r_sem,
                                            device_id=where, device_id_type=MESH)

    def kv_tile_src(t):
        per = kv_tiles // 2
        return (wk_hbm if t < per else wv_hbm).at[:, pl.ds((t % per) * TILE, TILE)]

    def tile_copy(src, slot):
        return pltpu.make_async_copy(src, wbuf.at[slot], tile_sem.at[slot])

    def q_tile_src(t):
        return wq_hbm.at[:, pl.ds(pl.multiple_of(t * TILE, TILE), TILE)]

    x_load = pltpu.make_async_copy(x_hbm, xbuf, load_sem.at[0])
    seg_load = pltpu.make_async_copy(seg_hbm, seg.at[me], load_sem.at[1])

    def rows_of(block, i):
        return pl.ds(pl.multiple_of(block * quarter + i * piece, piece), piece)

    def wo_piece_load(i):
        return pltpu.make_async_copy(wo_hbm.at[rows_of(me, i)], wo.at[rows_of(me, i)], load_sem.at[2 + i])

    def wo_rest_load(k, block):
        rows = pl.ds(pl.multiple_of(block * quarter, quarter), quarter)
        return pltpu.make_async_copy(wo_hbm.at[rows], wo.at[rows], load_sem.at[2 + pieces + k])

    others = (core_peer, chip_peer, far_peer)
    wo_piece_load(0).start()
    x_load.start()
    for t in range(kv_tiles):
        tile_copy(kv_tile_src(t), t).start()
    seg_load.start()

    barrier = pltpu.get_barrier_semaphore()
    for where in (tp_peer, at(core_peer), at(chip_peer), at(far_peer)):
        pl.semaphore_signal(barrier, inc=1, device_id=where, device_id_type=MESH)
    pl.semaphore_wait(barrier, 4)

    def y_copy(i):
        return remote((wo if i == 0 else wo_hbm).at[rows_of(me, i)], w_oth.at[rows_of(me, i)], y_s.at[i], y_r.at[i], tp_peer)

    def hand_on(block, i, s_sem, r_sem, where):
        part = w_oth.at[rows_of(block, i)]
        return remote(part, part, s_sem.at[i], r_sem.at[i], where)

    def seg_copy(k, block, where):
        return remote(seg.at[block], seg.at[block], seg_s.at[k], seg_r.at[k], where)

    def kv_copy(k, block, where):
        part = kv.at[:, pl.ds(pl.multiple_of(block * chunk, chunk), chunk), :]
        return remote(part, part, kv_s.at[k], kv_r.at[k], where)

    def o_copy(u):
        h = head_of(u)
        return remote(o_own.at[h], o_oth.at[h], o_s.at[u], o_r.at[u], tp_peer)

    def end_copy(r):
        h = head_of(heads - 1)
        rows = pl.ds(r * HEAD, HEAD)
        return remote(o_own.at[h, rows], o_oth.at[h, rows], o_s.at[heads - 1 + r], o_r.at[heads - 1 + r], tp_peer)

    def group_of(j):
        high = lax.rem(me // 2 + j // 2, 2)
        low = lax.rem(lax.rem(me, 2) + lax.rem(j, 2), 2)
        return 2 * high + low

    def place_of(u):
        half = u // 6
        v = u - 6 * half
        end = v // 4
        j = (1 - half) * (v // 3) + half * (2 + (1 - end) * (v // 2) + end * (v - 4))
        i = (1 - half) * (v % 3) + half * ((1 - end) * (v % 2) + 2 * end)
        return j, i

    def head_of(u):
        j, i = place_of(u)
        return group_of(j) * group + i

    wo_piece_load(0).wait()
    for i in range(pieces):
        y_copy(i).start()
    seg_load.wait()
    for k, block in enumerate(others):
        seg_copy(k, me, at(block)).start()

    x_load.wait()
    own_rows = pl.ds(pl.multiple_of(me * chunk, chunk), chunk)

    def project_kv(t, _):
        tile_copy(wk_hbm.at[:, pl.ds(0, TILE)], t).wait()
        part = jnp.dot(xbuf[...], wbuf[t], preferred_element_type=F32).astype(BF16)
        for k in range(TILE // HEAD):
            kv[t * (TILE // HEAD) + k, own_rows, :] = part[:, k * HEAD:(k + 1) * HEAD]

        @pl.when(t < q_tiles)
        def _():
            tile_copy(q_tile_src(t), t).start()
        return 0

    lax.fori_loop(0, kv_tiles, project_kv, 0)

    def project_q(t, _):
        slot = lax.rem(t, slots)
        tile_copy(q_tile_src(t), slot).wait()
        part = jnp.dot(xbuf[...], wbuf[slot], preferred_element_type=F32).astype(BF16)
        for k in range(TILE // HEAD):
            q[t * (TILE // HEAD) + k] = part[:, k * HEAD:(k + 1) * HEAD]

        @pl.when(t + slots < q_tiles)
        def _():
            tile_copy(q_tile_src(t + slots), slot).start()

        @pl.when(t == 0)
        def _():
            @pl.when(me < 2)
            def _():
                kv_copy(0, me, at(chip_peer)).start()
            kv_copy(1, me, at(core_peer)).start()
            for i in range(1, pieces):
                wo_piece_load(i).start()
            for k, block in enumerate(others):
                wo_rest_load(k, block).start()
        return 0

    lax.fori_loop(0, q_tiles, project_q, 0)

    def pass_y(i):
        y_copy(i).wait_recv()
        hand_on(me, i, xf_s, xf_r, at(chip_peer)).start()
        hand_on(me, i, d1_s, d1_r, at(core_peer)).start()

    def pass_x(i):
        hand_on(chip_peer, i, xf_s, xf_r, at(chip_peer)).wait_recv()
        hand_on(chip_peer, i, d2_s, d2_r, at(core_peer)).start()

    pass_y(0)
    for k, block in enumerate(others):
        seg_copy(k, block, at(block)).wait_recv()
    seg_col = jnp.transpose(jnp.broadcast_to(seg[me], (HEAD, chunk)))
    segq[...] = seg_col

    kv_copy(1, core_peer, at(core_peer)).wait_recv()

    @pl.when(me >= 2)
    def _():
        kv_copy(0, chip_peer, at(chip_peer)).wait_recv()
        kv_copy(2, chip_peer, at(core_peer)).start()
        kv_copy(2, far_peer, at(core_peer)).wait_recv()

    def attend(h, g, r, n):
        rows = pl.ds(pl.multiple_of(r * TILE, TILE), TILE)
        q_t = q[h, rows, :]
        sq = segq[rows, :]
        sq = jnp.concatenate([sq] * (chunk // HEAD), axis=1)
        parts = []
        for b in range(n):
            s = lax.dot_general(q_t, kv[g, pl.ds(b * chunk, chunk), :], (((1,), (1,)), ((), ())), preferred_element_type=F32)
            ok = sq == seg[b]
            if b == n - 1:
                q_pos = r * TILE + lax.broadcasted_iota(jnp.int32, (TILE, chunk), 0)
                ok = ok & (q_pos >= lax.broadcasted_iota(jnp.int32, (TILE, chunk), 1))
            parts.append(jnp.where(ok, s, -jnp.inf))
        top = parts[0].max(axis=1, keepdims=True)
        for s in parts[1:]:
            top = jnp.maximum(top, s.max(axis=1, keepdims=True))
        total = None
        acc = None
        for b, s in enumerate(parts):
            p = jnp.exp2((s - top) * SCALE)
            row_sum = p.sum(axis=1, keepdims=True)
            pv = jnp.dot(p.astype(BF16), kv[kv_heads + g, pl.ds(b * chunk, chunk), :], preferred_element_type=F32)
            total = row_sum if total is None else total + row_sum
            acc = pv if acc is None else acc + pv
        o_own[h, rows, :] = (acc / total).astype(BF16)

    def attend_head(u, _):
        h = head_of(u)
        g = h // group
        for n in range(1, n_blocks + 1):
            @pl.when(me == n - 1)
            def _(n=n):
                def one(r, c):
                    attend(h, g, r, n)
                    return c
                lax.fori_loop(0, chunk // TILE, one, 0)

        @pl.when(u > 0)
        def _():
            o_copy(u - 1).start()

        @pl.when(u == group - 1)
        def _():
            pass_y(1)

        @pl.when(u == 3 * group - 1)
        def _():
            pass_x(0)
        return 0

    lax.fori_loop(0, heads, attend_head, 0)
    pass_y(2)

    def add_rows(o_ref, w_ref, y_ref, h0, count, first):
        rows = pl.ds(pl.multiple_of(h0 * HEAD, HEAD), count * HEAD)

        def one(c, carry):
            cols = pl.ds(pl.multiple_of(c * COLS, COLS), COLS)
            left = jnp.concatenate([o_ref[h0 + k] for k in range(count)], axis=1)
            part = jnp.dot(left, w_ref[rows, cols], preferred_element_type=F32)
            y_ref[:, cols] = part if first else y_ref[:, cols] + part
            return carry

        lax.fori_loop(0, n_cols, one, 0)

    for i in range(1, pieces):
        wo_piece_load(i).wait()
    for k, block in enumerate(others):
        wo_rest_load(k, block).wait()
    runs = ((0, 3), (3, 3), (6, 2), (8, 2), (10, 1))
    for u, count in runs:
        add_rows(o_own, wo, y_own, head_of(u), count, u == 0)
        if u == 0:
            for r in range(ends):
                end_copy(r).start()
    add_rows(o_own, wo, y_own, head_of(heads - 1), 1, False)

    pass_x(1)
    for u, count in runs:
        for k in range(u, u + count):
            o_copy(k).wait_recv()
        if u == 3:
            for i in range(pieces):
                hand_on(core_peer, i, d1_s, d1_r, at(core_peer)).wait_recv()
        if u == 8:
            for i in range(pieces - 1):
                hand_on(far_peer, i, d2_s, d2_r, at(core_peer)).wait_recv()
        if u == 10:
            pass_x(2)
        add_rows(o_oth, w_oth, y_oth, head_of(u), count, u == 0)
    hand_on(far_peer, pieces - 1, d2_s, d2_r, at(core_peer)).wait_recv()

    h_end = head_of(heads - 1)
    w_end = pl.ds(pl.multiple_of(h_end * HEAD, HEAD), HEAD)
    for r in range(ends):
        rows = pl.ds(r * HEAD, HEAD)
        end_copy(r).wait_recv()

        for c in range(n_cols):
            cols = pl.ds(c * COLS, COLS)
            part = jnp.dot(o_oth[h_end, rows, :], w_oth[w_end, cols], preferred_element_type=F32)
            y_out[rows, cols] = (y_own[rows, cols] + (y_oth[rows, cols] + part)).astype(BF16)

    for i in range(pieces):
        y_copy(i).wait_send()
        hand_on(me, i, xf_s, xf_r, at(chip_peer)).wait_send()
        hand_on(me, i, d1_s, d1_r, at(core_peer)).wait_send()
        hand_on(chip_peer, i, d2_s, d2_r, at(core_peer)).wait_send()
    for k, block in enumerate(others):
        seg_copy(k, me, at(block)).wait_send()
    kv_copy(1, me, at(core_peer)).wait_send()

    @pl.when(me < 2)
    def _():
        kv_copy(0, me, at(chip_peer)).wait_send()

    @pl.when(me >= 2)
    def _():
        kv_copy(2, chip_peer, at(core_peer)).wait_send()

    for u in range(heads - 1):
        o_copy(u).wait_send()
    for r in range(ends):
        end_copy(r).wait_send()


def solution(mesh):
    n_blocks = mesh.shape['cp']

    def layer(x_loc, seg_loc, w_query, w_key, w_value, w_out):
        chunk, width = x_loc.shape
        kv_heads = w_key.shape[1] // HEAD
        heads = w_query.shape[1] // HEAD
        pieces = 3
        dma = pltpu.SemaphoreType.DMA
        any_spec = pl.BlockSpec(memory_space=pl.ANY)
        return pl.pallas_call(
            layer_kernel,
            out_shape=pltpu.VMEM((chunk, width), BF16),
            in_specs=[any_spec] * 6,
            out_specs=pl.BlockSpec(memory_space=pltpu.VMEM),
            scratch_shapes=[
                pltpu.VMEM((n_blocks, 1, chunk), jnp.int32),
                pltpu.VMEM((chunk, HEAD), jnp.int32),
                pltpu.VMEM((chunk, width), BF16),
                pltpu.VMEM((4, width, TILE), BF16),
                pltpu.VMEM((2 * kv_heads, n_blocks * chunk, HEAD), BF16),
                pltpu.VMEM((heads, chunk, HEAD), BF16),
                pltpu.VMEM((heads, chunk, HEAD), BF16),
                pltpu.VMEM((heads, chunk, HEAD), BF16),
                pltpu.VMEM(w_out.shape, BF16),
                pltpu.VMEM(w_out.shape, BF16),
                pltpu.VMEM((chunk, width), F32),
                pltpu.VMEM((chunk, width), F32),
                dma((5 + pieces,)), dma((4,)),
                dma((3,)), dma((3,)), dma((3,)), dma((3,)),
                dma((pieces,)), dma((pieces,)), dma((pieces,)), dma((pieces,)),
                dma((pieces,)), dma((pieces,)), dma((pieces,)), dma((pieces,)),
                dma((heads - 1 + chunk // HEAD,)), dma((heads - 1 + chunk // HEAD,)),
            ],
            compiler_params=pltpu.CompilerParams(collective_id=0, has_side_effects=True, vmem_limit_bytes=58 * 2 ** 20),
        )(seg_loc.reshape(1, chunk), x_loc, w_query, w_key, w_value, w_out)

    rows = P(('dp', 'cp'), None)
    return jax.shard_map(layer, mesh=mesh,
                         in_specs=(rows, P(('dp', 'cp')), P(None, 'tp'), P(None, 'tp'), P(None, 'tp'), P('tp', None)),
                         out_specs=rows, check_vma=False)
```

```python
import functools
import math

import jax
import jax.numpy as jnp
from jax import lax
from jax.experimental import pallas as pl
from jax.experimental.pallas import tpu as pltpu
from jax.sharding import PartitionSpec as P

HEAD = 128
TILE = 256
COLS = 512
MESH = pl.DeviceIdType.MESH
F32 = jnp.float32
BF16 = jnp.bfloat16
SCALE = HEAD ** -0.5 * math.log2(math.e)


def layer_kernel(seg_hbm, x_hbm, wq_hbm, wk_hbm, wv_hbm, wo_hbm,
                 y_own, y_oth, o_oth, w_oth,
                 seg, segq, xbuf, wbuf, kv, q, o_own, wo,
                 load_sem, tile_sem, seg_s, seg_r, kv_s, kv_r,
                 y_s, y_r, xf_s, xf_r, d1_s, d1_r, d2_s, d2_r, o_s, o_r):
    chunk, width = xbuf.shape
    kv_heads = kv.shape[0] // 2
    heads = q.shape[0]
    group = heads // kv_heads
    n_blocks = seg.shape[0]
    quarter = wo.shape[0] // n_blocks
    pieces = y_s.shape[0]
    piece = quarter // pieces
    n_cols = width // COLS
    kv_tiles = 2 * kv_heads * HEAD // TILE
    q_tiles = heads * HEAD // TILE
    slots = wbuf.shape[0]

    dp = lax.axis_index('dp')
    tp = lax.axis_index('tp')
    me = lax.axis_index('cp')
    core_peer = me + 1 - 2 * lax.rem(me, 2)
    chip_peer = lax.rem(me + 2, 4)
    far_peer = 3 - me
    others = (core_peer, chip_peer, far_peer)
    tp_peer = (dp, 1 - tp, me)

    def at(block):
        return (dp, tp, block)

    def remote(src, dst, s_sem, r_sem, where):
        return pltpu.make_async_remote_copy(src_ref=src, dst_ref=dst, send_sem=s_sem, recv_sem=r_sem,
                                            device_id=where, device_id_type=MESH)

    barrier = pltpu.get_barrier_semaphore()
    for where in (tp_peer, at(core_peer), at(chip_peer), at(far_peer)):
        pl.semaphore_signal(barrier, inc=1, device_id=where, device_id_type=MESH)

    def kv_tile_src(t):
        per = kv_tiles // 2
        return (wk_hbm if t < per else wv_hbm).at[:, pl.ds((t % per) * TILE, TILE)]

    def tile_copy(src, slot):
        return pltpu.make_async_copy(src, wbuf.at[slot], tile_sem.at[slot])

    def q_tile_src(t):
        return wq_hbm.at[:, pl.ds(pl.multiple_of(t * TILE, TILE), TILE)]

    x_load = pltpu.make_async_copy(x_hbm, xbuf, load_sem.at[0])
    wo_load = pltpu.make_async_copy(wo_hbm, wo, load_sem.at[2])
    seg_load = pltpu.make_async_copy(seg_hbm, seg.at[me], load_sem.at[1])

    x_load.start()
    for t in range(kv_tiles):
        tile_copy(kv_tile_src(t), t).start()
    seg_load.start()

    pl.semaphore_wait(barrier, 4)

    def rows_of(block, i):
        return pl.ds(pl.multiple_of(block * quarter + i * piece, piece), piece)

    def y_copy(i):
        return remote(wo_hbm.at[rows_of(me, i)], w_oth.at[rows_of(me, i)], y_s.at[i], y_r.at[i], tp_peer)

    def hand_on(block, i, s_sem, r_sem, where):
        part = w_oth.at[rows_of(block, i)]
        return remote(part, part, s_sem.at[i], r_sem.at[i], where)

    def seg_copy(k, block, where):
        return remote(seg.at[block], seg.at[block], seg_s.at[k], seg_r.at[k], where)

    def kv_copy(k, block, where):
        part = kv.at[:, pl.ds(pl.multiple_of(block * chunk, chunk), chunk), :]
        return remote(part, part, kv_s.at[k], kv_r.at[k], where)

    def o_copy(u):
        h = head_of(u)
        return remote(o_own.at[h], o_oth.at[h], o_s.at[u], o_r.at[u], tp_peer)

    def group_of(j):
        high = lax.rem(me // 2 + j // 2, 2)
        low = lax.rem(lax.rem(me, 2) + lax.rem(j, 2), 2)
        return 2 * high + low

    def place_of(u):
        half = u // 6
        v = u - 6 * half
        end = v // 4
        j = (1 - half) * (v // 3) + half * (2 + (1 - end) * (v // 2) + end * (v - 4))
        i = (1 - half) * (v % 3) + half * ((1 - end) * (v % 2) + 2 * end)
        return j, i

    def head_of(u):
        j, i = place_of(u)
        return group_of(j) * group + i

    for i in range(pieces):
        y_copy(i).start()
    seg_load.wait()
    for k, block in enumerate(others):
        seg_copy(k, me, at(block)).start()

    x_load.wait()
    own_rows = pl.ds(pl.multiple_of(me * chunk, chunk), chunk)

    def project_kv(t, _):
        tile_copy(wk_hbm.at[:, pl.ds(0, TILE)], t).wait()
        part = jnp.dot(xbuf[...], wbuf[t], preferred_element_type=F32).astype(BF16)
        for k in range(TILE // HEAD):
            kv[t * (TILE // HEAD) + k, own_rows, :] = part[:, k * HEAD:(k + 1) * HEAD]

        @pl.when(t < q_tiles)
        def _():
            tile_copy(q_tile_src(t), t).start()
        return 0

    lax.fori_loop(0, kv_tiles, project_kv, 0)

    def project_q(t, _):
        slot = lax.rem(t, slots)
        tile_copy(q_tile_src(t), slot).wait()
        part = jnp.dot(xbuf[...], wbuf[slot], preferred_element_type=F32).astype(BF16)
        for k in range(TILE // HEAD):
            q[t * (TILE // HEAD) + k] = part[:, k * HEAD:(k + 1) * HEAD]

        @pl.when(t + slots < q_tiles)
        def _():
            tile_copy(q_tile_src(t + slots), slot).start()

        @pl.when(t == 0)
        def _():
            @pl.when(me < 2)
            def _():
                kv_copy(0, me, at(chip_peer)).start()
            kv_copy(1, me, at(core_peer)).start()
            wo_load.start()
        return 0

    lax.fori_loop(0, q_tiles, project_q, 0)

    def pass_y(i):
        y_copy(i).wait_recv()
        hand_on(me, i, xf_s, xf_r, at(chip_peer)).start()
        hand_on(me, i, d1_s, d1_r, at(core_peer)).start()

    def pass_x(i):
        hand_on(chip_peer, i, xf_s, xf_r, at(chip_peer)).wait_recv()
        hand_on(chip_peer, i, d2_s, d2_r, at(core_peer)).start()

    pass_y(0)
    for k, block in enumerate(others):
        seg_copy(k, block, at(block)).wait_recv()
    seg_col = jnp.transpose(jnp.broadcast_to(seg[me], (HEAD, chunk)))
    segq[...] = seg_col

    kv_copy(1, core_peer, at(core_peer)).wait_recv()

    @pl.when(me >= 2)
    def _():
        kv_copy(0, chip_peer, at(chip_peer)).wait_recv()
        kv_copy(2, chip_peer, at(core_peer)).start()
        kv_copy(2, far_peer, at(core_peer)).wait_recv()

    def attend(h, g, r, n):
        rows = pl.ds(pl.multiple_of(r * TILE, TILE), TILE)
        q_t = q[h, rows, :]
        sq = segq[rows, :]
        sq = jnp.concatenate([sq] * (chunk // HEAD), axis=1)
        parts = []
        for b in range(n):
            s = lax.dot_general(q_t, kv[g, pl.ds(b * chunk, chunk), :], (((1,), (1,)), ((), ())), preferred_element_type=F32)
            ok = sq == seg[b]
            if b == n - 1:
                q_pos = r * TILE + lax.broadcasted_iota(jnp.int32, (TILE, chunk), 0)
                ok = ok & (q_pos >= lax.broadcasted_iota(jnp.int32, (TILE, chunk), 1))
            parts.append(jnp.where(ok, s, -jnp.inf))
        top = parts[0].max(axis=1, keepdims=True)
        for s in parts[1:]:
            top = jnp.maximum(top, s.max(axis=1, keepdims=True))
        total = None
        acc = None
        for b, s in enumerate(parts):
            p = jnp.exp2((s - top) * SCALE)
            row_sum = p.sum(axis=1, keepdims=True)
            pv = jnp.dot(p.astype(BF16), kv[kv_heads + g, pl.ds(b * chunk, chunk), :], preferred_element_type=F32)
            total = row_sum if total is None else total + row_sum
            acc = pv if acc is None else acc + pv
        o_own[h, rows, :] = (acc / total).astype(BF16)

    def attend_head(u, _):
        h = head_of(u)
        g = h // group
        for n in range(1, n_blocks + 1):
            @pl.when(me == n - 1)
            def _(n=n):
                def one(r, c):
                    attend(h, g, r, n)
                    return c
                lax.fori_loop(0, chunk // TILE, one, 0)

        @pl.when(u > 0)
        def _():
            o_copy(u - 1).start()

        @pl.when(u == group - 1)
        def _():
            pass_y(1)

        @pl.when(u == 3 * group - 1)
        def _():
            pass_x(0)
        return 0

    lax.fori_loop(0, heads, attend_head, 0)
    pass_y(2)

    def add_rows(o_ref, w_ref, y_ref, h0, count, first):
        rows = pl.ds(pl.multiple_of(h0 * HEAD, HEAD), count * HEAD)

        def one(c, carry):
            cols = pl.ds(pl.multiple_of(c * COLS, COLS), COLS)
            left = jnp.concatenate([o_ref[h0 + k] for k in range(count)], axis=1)
            part = jnp.dot(left, w_ref[rows, cols], preferred_element_type=F32)
            y_ref[:, cols] = part if first else y_ref[:, cols] + part
            return carry

        lax.fori_loop(0, n_cols, one, 0)

    wo_load.wait()
    runs = ((0, 3), (3, 3), (6, 2), (8, 2), (10, 1))
    for u, count in runs:
        add_rows(o_own, wo, y_own, head_of(u), count, u == 0)
        if u == 0:
            o_copy(heads - 1).start()
    add_rows(o_own, wo, y_own, head_of(heads - 1), 1, False)

    pass_x(1)
    for u, count in runs:
        for k in range(u, u + count):
            o_copy(k).wait_recv()
        if u == 3:
            for i in range(pieces):
                hand_on(core_peer, i, d1_s, d1_r, at(core_peer)).wait_recv()
        if u == 8:
            for i in range(pieces - 1):
                hand_on(far_peer, i, d2_s, d2_r, at(core_peer)).wait_recv()
        if u == 10:
            pass_x(2)
        add_rows(o_oth, w_oth, y_oth, head_of(u), count, u == 0)
    hand_on(far_peer, pieces - 1, d2_s, d2_r, at(core_peer)).wait_recv()

    o_copy(heads - 1).wait_recv()

    for i in range(pieces):
        y_copy(i).wait_send()
        hand_on(me, i, xf_s, xf_r, at(chip_peer)).wait_send()
        hand_on(me, i, d1_s, d1_r, at(core_peer)).wait_send()
        hand_on(chip_peer, i, d2_s, d2_r, at(core_peer)).wait_send()
    for k, block in enumerate(others):
        seg_copy(k, me, at(block)).wait_send()
    kv_copy(1, me, at(core_peer)).wait_send()

    @pl.when(me < 2)
    def _():
        kv_copy(0, me, at(chip_peer)).wait_send()

    @pl.when(me >= 2)
    def _():
        kv_copy(2, chip_peer, at(core_peer)).wait_send()

    for u in range(heads):
        o_copy(u).wait_send()


def last_kernel(last_head, y_own, y_oth, o_oth, w_oth, y_hbm, y_out, out_sem):
    h = last_head(lax.axis_index('cp'))
    left = o_oth[h]
    rows = pl.ds(pl.multiple_of(h * HEAD, HEAD), HEAD)
    copies = []
    for c in range(y_out.shape[1] // COLS):
        cols = pl.ds(c * COLS, COLS)
        part = jnp.dot(left, w_oth[rows, cols], preferred_element_type=F32)
        y_out[:, cols] = (y_own[:, cols] + (y_oth[:, cols] + part)).astype(BF16)
        copy = pltpu.make_async_copy(y_out.at[:, cols], y_hbm.at[:, cols], out_sem.at[c])
        copy.start()
        copies.append(copy)
    for copy in copies:
        copy.wait()


def solution(mesh):
    n_blocks = mesh.shape['cp']

    def layer(x_loc, seg_loc, w_query, w_key, w_value, w_out):
        chunk, width = x_loc.shape
        kv_heads = w_key.shape[1] // HEAD
        heads = w_query.shape[1] // HEAD
        pieces = 3
        dma = pltpu.SemaphoreType.DMA
        any_spec = pl.BlockSpec(memory_space=pl.ANY)
        vmem_spec = pl.BlockSpec(memory_space=pltpu.VMEM)
        parts = pl.pallas_call(
            layer_kernel,
            out_shape=(
                pltpu.VMEM((chunk, width), F32),
                pltpu.VMEM((chunk, width), F32),
                pltpu.VMEM((heads, chunk, HEAD), BF16),
                pltpu.VMEM(w_out.shape, BF16),
            ),
            in_specs=[any_spec] * 6,
            out_specs=[vmem_spec] * 4,
            scratch_shapes=[
                pltpu.VMEM((n_blocks, 1, chunk), jnp.int32),
                pltpu.VMEM((chunk, HEAD), jnp.int32),
                pltpu.VMEM((chunk, width), BF16),
                pltpu.VMEM((4, width, TILE), BF16),
                pltpu.VMEM((2 * kv_heads, n_blocks * chunk, HEAD), BF16),
                pltpu.VMEM((heads, chunk, HEAD), BF16),
                pltpu.VMEM((heads, chunk, HEAD), BF16),
                pltpu.VMEM(w_out.shape, BF16),
                dma((3,)), dma((4,)),
                dma((3,)), dma((3,)), dma((3,)), dma((3,)),
                dma((pieces,)), dma((pieces,)), dma((pieces,)), dma((pieces,)),
                dma((pieces,)), dma((pieces,)), dma((pieces,)), dma((pieces,)),
                dma((heads,)), dma((heads,)),
            ],
            compiler_params=pltpu.CompilerParams(collective_id=0, has_side_effects=True, vmem_limit_bytes=36 * 2 ** 20),
        )(seg_loc.reshape(1, chunk), x_loc, w_query, w_key, w_value, w_out)
        parts = [pltpu.with_memory_space_constraint(a, pltpu.VMEM) for a in parts]

        def last_head(me):
            return (3 - me) * (heads // kv_heads) + heads // kv_heads - 1

        return pl.pallas_call(
            functools.partial(last_kernel, last_head),
            out_shape=jax.ShapeDtypeStruct((chunk, width), BF16),
            in_specs=[vmem_spec] * 4,
            out_specs=any_spec,
            scratch_shapes=[pltpu.VMEM((chunk, width), BF16), dma((width // COLS,))],
            compiler_params=pltpu.CompilerParams(vmem_limit_bytes=8 * 2 ** 20),
        )(*parts)

    rows = P(('dp', 'cp'), None)
    return jax.shard_map(layer, mesh=mesh,
                         in_specs=(rows, P(('dp', 'cp')), P(None, 'tp'), P(None, 'tp'), P(None, 'tp'), P('tp', None)),
                         out_specs=rows, check_vma=False)
```

```python
import functools
import math

import jax
import jax.numpy as jnp
from jax import lax
from jax.experimental import pallas as pl
from jax.experimental.pallas import tpu as pltpu
from jax.sharding import PartitionSpec as P

HEAD = 128
TILE = 256
COLS = 512
MESH = pl.DeviceIdType.MESH
F32 = jnp.float32
BF16 = jnp.bfloat16
SCALE = HEAD ** -0.5 * math.log2(math.e)


def layer_kernel(seg_hbm, x_hbm, wq_hbm, wk_hbm, wv_hbm, wo_hbm,
                 y_own, y_oth, o_oth, w_oth,
                 seg, segq, xbuf, wbuf, kv, q, o_own, wo,
                 entry, load_sem, tile_sem, seg_s, seg_r, kv_s, kv_r,
                 y_s, y_r, xf_s, xf_r, d1_s, d1_r, d2_s, d2_r, o_s, o_r):
    chunk, width = xbuf.shape
    kv_heads = kv.shape[0] // 2
    heads = q.shape[0]
    group = heads // kv_heads
    n_blocks = seg.shape[0]
    quarter = wo.shape[0] // n_blocks
    pieces = y_s.shape[0]
    piece = quarter // pieces
    n_cols = width // COLS
    kv_tiles = 2 * kv_heads * HEAD // TILE
    q_tiles = heads * HEAD // TILE
    slots = wbuf.shape[0]

    dp = lax.axis_index('dp')
    tp = lax.axis_index('tp')
    me = lax.axis_index('cp')
    core_peer = me + 1 - 2 * lax.rem(me, 2)
    chip_peer = lax.rem(me + 2, 4)
    far_peer = 3 - me
    others = (core_peer, chip_peer, far_peer)
    tp_peer = (dp, 1 - tp, me)

    def at(block):
        return (dp, tp, block)

    def remote(src, dst, s_sem, r_sem, where):
        return pltpu.make_async_remote_copy(src_ref=src, dst_ref=dst, send_sem=s_sem, recv_sem=r_sem,
                                            device_id=where, device_id_type=MESH)

    odd = lax.rem(me, 2)
    barrier = pltpu.get_barrier_semaphore()
    for where in (tp_peer, at(core_peer)):
        pl.semaphore_signal(barrier, inc=1, device_id=where, device_id_type=MESH)

    @pl.when(odd == 1)
    def _():
        pl.semaphore_signal(barrier, inc=1, device_id=at(chip_peer), device_id_type=MESH)

    def kv_tile_src(t):
        per = kv_tiles // 2
        return (wk_hbm if t < per else wv_hbm).at[:, pl.ds((t % per) * TILE, TILE)]

    def tile_copy(src, slot):
        return pltpu.make_async_copy(src, wbuf.at[slot], tile_sem.at[slot])

    def q_tile_src(t):
        return wq_hbm.at[:, pl.ds(pl.multiple_of(t * TILE, TILE), TILE)]

    x_load = pltpu.make_async_copy(x_hbm, xbuf, load_sem.at[0])
    wo_load = pltpu.make_async_copy(wo_hbm, wo, load_sem.at[2])
    seg_load = pltpu.make_async_copy(seg_hbm, seg.at[me], load_sem.at[1])

    x_load.start()
    for t in range(kv_tiles):
        tile_copy(kv_tile_src(t), t).start()
    seg_load.start()


    def rows_of(block, i):
        return pl.ds(pl.multiple_of(block * quarter + i * piece, piece), piece)

    def y_copy(i):
        return remote(wo_hbm.at[rows_of(me, i)], w_oth.at[rows_of(me, i)], y_s.at[i], y_r.at[i], tp_peer)

    def hand_on(block, i, s_sem, r_sem, where):
        part = w_oth.at[rows_of(block, i)]
        return remote(part, part, s_sem.at[i], r_sem.at[i], where)

    def seg_copy(k, block, where):
        return remote(seg.at[block], seg.at[block], seg_s.at[k], seg_r.at[k], where)

    def kv_copy(k, block, where):
        part = kv.at[:, pl.ds(pl.multiple_of(block * chunk, chunk), chunk), :]
        return remote(part, part, kv_s.at[k], kv_r.at[k], where)

    def o_copy(u):
        h = head_of(u)
        return remote(o_own.at[h], o_oth.at[h], o_s.at[u], o_r.at[u], tp_peer)

    def group_of(j):
        high = lax.rem(me // 2 + j // 2, 2)
        low = lax.rem(lax.rem(me, 2) + lax.rem(j, 2), 2)
        return 2 * high + low

    def place_of(u):
        half = u // 6
        v = u - 6 * half
        end = v // 4
        j = (1 - half) * (v // 3) + half * (2 + (1 - end) * (v // 2) + end * (v - 4))
        i = (1 - half) * (v % 3) + half * ((1 - end) * (v % 2) + 2 * end)
        return j, i

    def head_of(u):
        j, i = place_of(u)
        return group_of(j) * group + i

    pl.semaphore_wait(barrier, 2 + odd)
    for i in range(pieces):
        y_copy(i).start()

    @pl.when(odd == 1)
    def _():
        pl.semaphore_signal(entry, inc=1, device_id=at(chip_peer), device_id_type=MESH)
        pl.semaphore_wait(entry, 1)
        pl.semaphore_signal(entry, inc=1, device_id=at(core_peer), device_id_type=MESH)

    @pl.when(odd == 0)
    def _():
        pl.semaphore_wait(entry, 1)

    seg_load.wait()
    for k, block in enumerate(others):
        seg_copy(k, me, at(block)).start()

    x_load.wait()
    own_rows = pl.ds(pl.multiple_of(me * chunk, chunk), chunk)

    def project_kv(t, _):
        tile_copy(wk_hbm.at[:, pl.ds(0, TILE)], t).wait()
        part = jnp.dot(xbuf[...], wbuf[t], preferred_element_type=F32).astype(BF16)
        for k in range(TILE // HEAD):
            kv[t * (TILE // HEAD) + k, own_rows, :] = part[:, k * HEAD:(k + 1) * HEAD]

        @pl.when(t < q_tiles)
        def _():
            tile_copy(q_tile_src(t), t).start()
        return 0

    lax.fori_loop(0, kv_tiles, project_kv, 0)

    def project_q(t, _):
        slot = lax.rem(t, slots)
        tile_copy(q_tile_src(t), slot).wait()
        part = jnp.dot(xbuf[...], wbuf[slot], preferred_element_type=F32).astype(BF16)
        for k in range(TILE // HEAD):
            q[t * (TILE // HEAD) + k] = part[:, k * HEAD:(k + 1) * HEAD]

        @pl.when(t + slots < q_tiles)
        def _():
            tile_copy(q_tile_src(t + slots), slot).start()

        @pl.when(t == 0)
        def _():
            @pl.when(me < 2)
            def _():
                kv_copy(0, me, at(chip_peer)).start()
            kv_copy(1, me, at(core_peer)).start()
            wo_load.start()
        return 0

    lax.fori_loop(0, q_tiles, project_q, 0)

    def pass_y(i):
        y_copy(i).wait_recv()
        hand_on(me, i, xf_s, xf_r, at(chip_peer)).start()
        hand_on(me, i, d1_s, d1_r, at(core_peer)).start()

    def pass_x(i):
        hand_on(chip_peer, i, xf_s, xf_r, at(chip_peer)).wait_recv()
        hand_on(chip_peer, i, d2_s, d2_r, at(core_peer)).start()

    pass_y(0)
    for k, block in enumerate(others):
        seg_copy(k, block, at(block)).wait_recv()
    seg_col = jnp.transpose(jnp.broadcast_to(seg[me], (HEAD, chunk)))
    segq[...] = seg_col

    kv_copy(1, core_peer, at(core_peer)).wait_recv()

    @pl.when(me >= 2)
    def _():
        kv_copy(0, chip_peer, at(chip_peer)).wait_recv()
        kv_copy(2, chip_peer, at(core_peer)).start()
        kv_copy(2, far_peer, at(core_peer)).wait_recv()

    def attend(h, g, r, n):
        rows = pl.ds(pl.multiple_of(r * TILE, TILE), TILE)
        q_t = q[h, rows, :]
        sq = segq[rows, :]
        sq = jnp.concatenate([sq] * (chunk // HEAD), axis=1)
        parts = []
        for b in range(n):
            s = lax.dot_general(q_t, kv[g, pl.ds(b * chunk, chunk), :], (((1,), (1,)), ((), ())), preferred_element_type=F32)
            ok = sq == seg[b]
            if b == n - 1:
                q_pos = r * TILE + lax.broadcasted_iota(jnp.int32, (TILE, chunk), 0)
                ok = ok & (q_pos >= lax.broadcasted_iota(jnp.int32, (TILE, chunk), 1))
            parts.append(jnp.where(ok, s, -jnp.inf))
        top = parts[0].max(axis=1, keepdims=True)
        for s in parts[1:]:
            top = jnp.maximum(top, s.max(axis=1, keepdims=True))
        total = None
        acc = None
        for b, s in enumerate(parts):
            p = jnp.exp2((s - top) * SCALE)
            row_sum = p.sum(axis=1, keepdims=True)
            pv = jnp.dot(p.astype(BF16), kv[kv_heads + g, pl.ds(b * chunk, chunk), :], preferred_element_type=F32)
            total = row_sum if total is None else total + row_sum
            acc = pv if acc is None else acc + pv
        o_own[h, rows, :] = (acc / total).astype(BF16)

    def attend_head(u, _):
        h = head_of(u)
        g = h // group
        for n in range(1, n_blocks + 1):
            @pl.when(me == n - 1)
            def _(n=n):
                def one(r, c):
                    attend(h, g, r, n)
                    return c
                lax.fori_loop(0, chunk // TILE, one, 0)

        @pl.when(u > 0)
        def _():
            o_copy(u - 1).start()

        @pl.when(u == group - 1)
        def _():
            pass_y(1)

        @pl.when(u == 3 * group - 1)
        def _():
            pass_x(0)
        return 0

    lax.fori_loop(0, heads, attend_head, 0)
    pass_y(2)

    def add_rows(o_ref, w_ref, y_ref, h0, count, first):
        rows = pl.ds(pl.multiple_of(h0 * HEAD, HEAD), count * HEAD)

        def one(c, carry):
            cols = pl.ds(pl.multiple_of(c * COLS, COLS), COLS)
            left = jnp.concatenate([o_ref[h0 + k] for k in range(count)], axis=1)
            part = jnp.dot(left, w_ref[rows, cols], preferred_element_type=F32)
            y_ref[:, cols] = part if first else y_ref[:, cols] + part
            return carry

        lax.fori_loop(0, n_cols, one, 0)

    wo_load.wait()
    runs = ((0, 3), (3, 3), (6, 2), (8, 2), (10, 1))
    for u, count in runs:
        add_rows(o_own, wo, y_own, head_of(u), count, u == 0)
        if u == 0:
            o_copy(heads - 1).start()
    add_rows(o_own, wo, y_own, head_of(heads - 1), 1, False)

    pass_x(1)
    for u, count in runs:
        for k in range(u, u + count):
            o_copy(k).wait_recv()
        if u == 3:
            for i in range(pieces):
                hand_on(core_peer, i, d1_s, d1_r, at(core_peer)).wait_recv()
        if u == 8:
            for i in range(pieces - 1):
                hand_on(far_peer, i, d2_s, d2_r, at(core_peer)).wait_recv()
        if u == 10:
            pass_x(2)
        add_rows(o_oth, w_oth, y_oth, head_of(u), count, u == 0)
    hand_on(far_peer, pieces - 1, d2_s, d2_r, at(core_peer)).wait_recv()

    o_copy(heads - 1).wait_recv()

    for i in range(pieces):
        y_copy(i).wait_send()
        hand_on(me, i, xf_s, xf_r, at(chip_peer)).wait_send()
        hand_on(me, i, d1_s, d1_r, at(core_peer)).wait_send()
        hand_on(chip_peer, i, d2_s, d2_r, at(core_peer)).wait_send()
    for k, block in enumerate(others):
        seg_copy(k, me, at(block)).wait_send()
    kv_copy(1, me, at(core_peer)).wait_send()

    @pl.when(me < 2)
    def _():
        kv_copy(0, me, at(chip_peer)).wait_send()

    @pl.when(me >= 2)
    def _():
        kv_copy(2, chip_peer, at(core_peer)).wait_send()

    for u in range(heads):
        o_copy(u).wait_send()


def last_kernel(last_head, y_own, y_oth, o_oth, w_oth, y_hbm, y_out, out_sem):
    h = last_head(lax.axis_index('cp'))
    left = o_oth[h]
    rows = pl.ds(pl.multiple_of(h * HEAD, HEAD), HEAD)
    copies = []
    for c in range(y_out.shape[1] // COLS):
        cols = pl.ds(c * COLS, COLS)
        part = jnp.dot(left, w_oth[rows, cols], preferred_element_type=F32)
        y_out[:, cols] = (y_own[:, cols] + (y_oth[:, cols] + part)).astype(BF16)
        copy = pltpu.make_async_copy(y_out.at[:, cols], y_hbm.at[:, cols], out_sem.at[c])
        copy.start()
        copies.append(copy)
    for copy in copies:
        copy.wait()


def solution(mesh):
    n_blocks = mesh.shape['cp']

    def layer(x_loc, seg_loc, w_query, w_key, w_value, w_out):
        chunk, width = x_loc.shape
        kv_heads = w_key.shape[1] // HEAD
        heads = w_query.shape[1] // HEAD
        pieces = 3
        dma = pltpu.SemaphoreType.DMA
        any_spec = pl.BlockSpec(memory_space=pl.ANY)
        vmem_spec = pl.BlockSpec(memory_space=pltpu.VMEM)
        parts = pl.pallas_call(
            layer_kernel,
            out_shape=(
                pltpu.VMEM((chunk, width), F32),
                pltpu.VMEM((chunk, width), F32),
                pltpu.VMEM((heads, chunk, HEAD), BF16),
                pltpu.VMEM(w_out.shape, BF16),
            ),
            in_specs=[any_spec] * 6,
            out_specs=[vmem_spec] * 4,
            scratch_shapes=[
                pltpu.VMEM((n_blocks, 1, chunk), jnp.int32),
                pltpu.VMEM((chunk, HEAD), jnp.int32),
                pltpu.VMEM((chunk, width), BF16),
                pltpu.VMEM((4, width, TILE), BF16),
                pltpu.VMEM((2 * kv_heads, n_blocks * chunk, HEAD), BF16),
                pltpu.VMEM((heads, chunk, HEAD), BF16),
                pltpu.VMEM((heads, chunk, HEAD), BF16),
                pltpu.VMEM(w_out.shape, BF16),
                pltpu.SemaphoreType.REGULAR, dma((3,)), dma((4,)),
                dma((3,)), dma((3,)), dma((3,)), dma((3,)),
                dma((pieces,)), dma((pieces,)), dma((pieces,)), dma((pieces,)),
                dma((pieces,)), dma((pieces,)), dma((pieces,)), dma((pieces,)),
                dma((heads,)), dma((heads,)),
            ],
            compiler_params=pltpu.CompilerParams(collective_id=0, has_side_effects=True, vmem_limit_bytes=36 * 2 ** 20),
        )(seg_loc.reshape(1, chunk), x_loc, w_query, w_key, w_value, w_out)
        parts = [pltpu.with_memory_space_constraint(a, pltpu.VMEM) for a in parts]

        def last_head(me):
            return (3 - me) * (heads // kv_heads) + heads // kv_heads - 1

        return pl.pallas_call(
            functools.partial(last_kernel, last_head),
            out_shape=jax.ShapeDtypeStruct((chunk, width), BF16),
            in_specs=[vmem_spec] * 4,
            out_specs=any_spec,
            scratch_shapes=[pltpu.VMEM((chunk, width), BF16), dma((width // COLS,))],
            compiler_params=pltpu.CompilerParams(vmem_limit_bytes=8 * 2 ** 20),
        )(*parts)

    rows = P(('dp', 'cp'), None)
    return jax.shard_map(layer, mesh=mesh,
                         in_specs=(rows, P(('dp', 'cp')), P(None, 'tp'), P(None, 'tp'), P(None, 'tp'), P('tp', None)),
                         out_specs=rows, check_vma=False)
```

```python
import functools
import math

import jax
import jax.numpy as jnp
from jax import lax
from jax.experimental import pallas as pl
from jax.experimental.pallas import tpu as pltpu
from jax.sharding import PartitionSpec as P

HEAD = 128
TILE = 256
COLS = 512
SENDS = ((0, 3), (3, 3), (6, 2), (8, 2), (10, 1), (11, 1))
MESH = pl.DeviceIdType.MESH
F32 = jnp.float32
BF16 = jnp.bfloat16
SCALE = HEAD ** -0.5 * math.log2(math.e)


def layer_kernel(seg_hbm, x_hbm, wq_hbm, wk_hbm, wv_hbm, wo_hbm,
                 y_own, y_oth, o_oth, w_oth,
                 seg, segq, xbuf, wbuf, kv, q, o_own, wo,
                 entry, load_sem, tile_sem, seg_s, seg_r, kv_s, kv_r,
                 y_s, y_r, xf_s, xf_r, d1_s, d1_r, d2_s, d2_r, o_s, o_r):
    chunk, width = xbuf.shape
    kv_heads = kv.shape[0] // 2
    heads = q.shape[0]
    group = heads // kv_heads
    n_blocks = seg.shape[0]
    quarter = wo.shape[0] // n_blocks
    pieces = y_s.shape[0]
    piece = quarter // pieces
    n_cols = width // COLS
    kv_tiles = 2 * kv_heads * HEAD // TILE
    q_tiles = heads * HEAD // TILE
    slots = wbuf.shape[0]

    dp = lax.axis_index('dp')
    tp = lax.axis_index('tp')
    me = lax.axis_index('cp')
    core_peer = me + 1 - 2 * lax.rem(me, 2)
    chip_peer = lax.rem(me + 2, 4)
    far_peer = 3 - me
    others = (core_peer, chip_peer, far_peer)
    tp_peer = (dp, 1 - tp, me)

    def at(block):
        return (dp, tp, block)

    def remote(src, dst, s_sem, r_sem, where):
        return pltpu.make_async_remote_copy(src_ref=src, dst_ref=dst, send_sem=s_sem, recv_sem=r_sem,
                                            device_id=where, device_id_type=MESH)

    odd = lax.rem(me, 2)
    barrier = pltpu.get_barrier_semaphore()
    for where in (tp_peer, at(core_peer)):
        pl.semaphore_signal(barrier, inc=1, device_id=where, device_id_type=MESH)

    @pl.when(odd == 1)
    def _():
        pl.semaphore_signal(barrier, inc=1, device_id=at(chip_peer), device_id_type=MESH)

    def kv_tile_src(t):
        per = kv_tiles // 2
        return (wk_hbm if t < per else wv_hbm).at[:, pl.ds((t % per) * TILE, TILE)]

    def tile_copy(src, slot):
        return pltpu.make_async_copy(src, wbuf.at[slot], tile_sem.at[slot])

    def q_tile_src(t):
        return wq_hbm.at[:, pl.ds(pl.multiple_of(t * TILE, TILE), TILE)]

    x_load = pltpu.make_async_copy(x_hbm, xbuf, load_sem.at[0])
    wo_load = pltpu.make_async_copy(wo_hbm, wo, load_sem.at[2])
    seg_load = pltpu.make_async_copy(seg_hbm, seg.at[me], load_sem.at[1])

    x_load.start()
    for t in range(kv_tiles):
        tile_copy(kv_tile_src(t), t).start()
    seg_load.start()


    def rows_of(block, i):
        return pl.ds(pl.multiple_of(block * quarter + i * piece, piece), piece)

    def y_copy(i):
        return remote(wo_hbm.at[rows_of(me, i)], w_oth.at[rows_of(me, i)], y_s.at[i], y_r.at[i], tp_peer)

    def hand_on(block, i, s_sem, r_sem, where):
        part = w_oth.at[rows_of(block, i)]
        return remote(part, part, s_sem.at[i], r_sem.at[i], where)

    def seg_copy(k, block, where):
        return remote(seg.at[block], seg.at[block], seg_s.at[k], seg_r.at[k], where)

    def kv_copy(k, block, where):
        part = kv.at[:, pl.ds(pl.multiple_of(block * chunk, chunk), chunk), :]
        return remote(part, part, kv_s.at[k], kv_r.at[k], where)

    def o_copy(k):
        part = pl.ds(*SENDS[k])
        return remote(o_own.at[part], o_oth.at[part], o_s.at[k], o_r.at[k], tp_peer)

    def group_of(j):
        high = lax.rem(me // 2 + j // 2, 2)
        low = lax.rem(lax.rem(me, 2) + lax.rem(j, 2), 2)
        return 2 * high + low

    def place_of(u):
        half = u // 6
        v = u - 6 * half
        end = v // 4
        j = (1 - half) * (v // 3) + half * (2 + (1 - end) * (v // 2) + end * (v - 4))
        i = (1 - half) * (v % 3) + half * ((1 - end) * (v % 2) + 2 * end)
        return j, i

    def head_of(u):
        j, i = place_of(u)
        return group_of(j) * group + i

    pl.semaphore_wait(barrier, 2 + odd)
    for i in range(pieces):
        y_copy(i).start()

    @pl.when(odd == 1)
    def _():
        pl.semaphore_signal(entry, inc=1, device_id=at(chip_peer), device_id_type=MESH)
        pl.semaphore_wait(entry, 1)
        pl.semaphore_signal(entry, inc=1, device_id=at(core_peer), device_id_type=MESH)

    @pl.when(odd == 0)
    def _():
        pl.semaphore_wait(entry, 1)

    seg_load.wait()
    for k, block in enumerate(others):
        seg_copy(k, me, at(block)).start()

    x_load.wait()
    own_rows = pl.ds(pl.multiple_of(me * chunk, chunk), chunk)

    def project_kv(t, _):
        tile_copy(wk_hbm.at[:, pl.ds(0, TILE)], t).wait()
        part = jnp.dot(xbuf[...], wbuf[t], preferred_element_type=F32).astype(BF16)
        for k in range(TILE // HEAD):
            kv[t * (TILE // HEAD) + k, own_rows, :] = part[:, k * HEAD:(k + 1) * HEAD]

        @pl.when(t < q_tiles)
        def _():
            tile_copy(q_tile_src(t), t).start()
        return 0

    lax.fori_loop(0, kv_tiles, project_kv, 0)

    def project_q(t, _):
        slot = lax.rem(t, slots)
        tile_copy(q_tile_src(t), slot).wait()
        part = jnp.dot(xbuf[...], wbuf[slot], preferred_element_type=F32).astype(BF16)
        for k in range(TILE // HEAD):
            q[t * (TILE // HEAD) + k] = part[:, k * HEAD:(k + 1) * HEAD]

        @pl.when(t + slots < q_tiles)
        def _():
            tile_copy(q_tile_src(t + slots), slot).start()

        @pl.when(t == 0)
        def _():
            @pl.when(me < 2)
            def _():
                kv_copy(0, me, at(chip_peer)).start()
            kv_copy(1, me, at(core_peer)).start()
            wo_load.start()
        return 0

    lax.fori_loop(0, q_tiles, project_q, 0)

    def pass_y(i):
        y_copy(i).wait_recv()
        hand_on(me, i, xf_s, xf_r, at(chip_peer)).start()
        hand_on(me, i, d1_s, d1_r, at(core_peer)).start()

    def pass_x(i):
        hand_on(chip_peer, i, xf_s, xf_r, at(chip_peer)).wait_recv()
        hand_on(chip_peer, i, d2_s, d2_r, at(core_peer)).start()

    pass_y(0)
    for k, block in enumerate(others):
        seg_copy(k, block, at(block)).wait_recv()
    seg_col = jnp.transpose(jnp.broadcast_to(seg[me], (HEAD, chunk)))
    segq[...] = seg_col

    kv_copy(1, core_peer, at(core_peer)).wait_recv()

    @pl.when(me >= 2)
    def _():
        kv_copy(0, chip_peer, at(chip_peer)).wait_recv()
        kv_copy(2, chip_peer, at(core_peer)).start()
        kv_copy(2, far_peer, at(core_peer)).wait_recv()

    def attend(u, h, g, r, n):
        rows = pl.ds(pl.multiple_of(r * TILE, TILE), TILE)
        q_t = q[h, rows, :]
        sq = segq[rows, :]
        sq = jnp.concatenate([sq] * (chunk // HEAD), axis=1)
        parts = []
        for b in range(n):
            s = lax.dot_general(q_t, kv[g, pl.ds(b * chunk, chunk), :], (((1,), (1,)), ((), ())), preferred_element_type=F32)
            ok = sq == seg[b]
            if b == n - 1:
                q_pos = r * TILE + lax.broadcasted_iota(jnp.int32, (TILE, chunk), 0)
                ok = ok & (q_pos >= lax.broadcasted_iota(jnp.int32, (TILE, chunk), 1))
            parts.append(jnp.where(ok, s, -jnp.inf))
        top = parts[0].max(axis=1, keepdims=True)
        for s in parts[1:]:
            top = jnp.maximum(top, s.max(axis=1, keepdims=True))
        total = None
        acc = None
        for b, s in enumerate(parts):
            p = jnp.exp2((s - top) * SCALE)
            row_sum = p.sum(axis=1, keepdims=True)
            pv = jnp.dot(p.astype(BF16), kv[kv_heads + g, pl.ds(b * chunk, chunk), :], preferred_element_type=F32)
            total = row_sum if total is None else total + row_sum
            acc = pv if acc is None else acc + pv
        o_own[u, rows, :] = (acc / total).astype(BF16)

    def attend_head(u, _):
        h = head_of(u)
        g = h // group
        for n in range(1, n_blocks + 1):
            @pl.when(me == n - 1)
            def _(n=n):
                def one(r, c):
                    attend(u, h, g, r, n)
                    return c
                lax.fori_loop(0, chunk // TILE, one, 0)

        for k, (begin, count) in enumerate(SENDS[:-1]):
            @pl.when(u == begin + count)
            def _(k=k):
                o_copy(k).start()

        @pl.when(u == group - 1)
        def _():
            pass_y(1)

        @pl.when(u == 3 * group - 1)
        def _():
            pass_x(0)
        return 0

    lax.fori_loop(0, heads, attend_head, 0)
    pass_y(2)

    def add_rows(o_ref, w_ref, y_ref, u, count, first):
        rows = pl.ds(pl.multiple_of(head_of(u) * HEAD, HEAD), count * HEAD)

        def one(c, carry):
            cols = pl.ds(pl.multiple_of(c * COLS, COLS), COLS)
            left = jnp.concatenate([o_ref[u + k] for k in range(count)], axis=1)
            part = jnp.dot(left, w_ref[rows, cols], preferred_element_type=F32)
            y_ref[:, cols] = part if first else y_ref[:, cols] + part
            return carry

        lax.fori_loop(0, n_cols, one, 0)

    wo_load.wait()
    runs = ((0, 3), (3, 3), (6, 2), (8, 2), (10, 1))
    for u, count in runs:
        add_rows(o_own, wo, y_own, u, count, u == 0)
        if u == 0:
            o_copy(len(SENDS) - 1).start()
    add_rows(o_own, wo, y_own, heads - 1, 1, False)

    pass_x(1)
    for u, count in runs:
        for k, (begin, _) in enumerate(SENDS):
            if u <= begin < u + count:
                o_copy(k).wait_recv()
        if u == 3:
            for i in range(pieces):
                hand_on(core_peer, i, d1_s, d1_r, at(core_peer)).wait_recv()
        if u == 8:
            for i in range(pieces - 1):
                hand_on(far_peer, i, d2_s, d2_r, at(core_peer)).wait_recv()
        if u == 10:
            pass_x(2)
        add_rows(o_oth, w_oth, y_oth, u, count, u == 0)
    hand_on(far_peer, pieces - 1, d2_s, d2_r, at(core_peer)).wait_recv()

    o_copy(len(SENDS) - 1).wait_recv()

    for i in range(pieces):
        y_copy(i).wait_send()
        hand_on(me, i, xf_s, xf_r, at(chip_peer)).wait_send()
        hand_on(me, i, d1_s, d1_r, at(core_peer)).wait_send()
        hand_on(chip_peer, i, d2_s, d2_r, at(core_peer)).wait_send()
    for k, block in enumerate(others):
        seg_copy(k, me, at(block)).wait_send()
    kv_copy(1, me, at(core_peer)).wait_send()

    @pl.when(me < 2)
    def _():
        kv_copy(0, me, at(chip_peer)).wait_send()

    @pl.when(me >= 2)
    def _():
        kv_copy(2, chip_peer, at(core_peer)).wait_send()

    for k in range(len(SENDS)):
        o_copy(k).wait_send()


def last_kernel(last_head, y_own, y_oth, o_oth, w_oth, y_hbm, y_out, out_sem):
    h = last_head(lax.axis_index('cp'))
    left = o_oth[o_oth.shape[0] - 1]
    rows = pl.ds(pl.multiple_of(h * HEAD, HEAD), HEAD)
    copies = []
    for c in range(y_out.shape[1] // COLS):
        cols = pl.ds(c * COLS, COLS)
        part = jnp.dot(left, w_oth[rows, cols], preferred_element_type=F32)
        y_out[:, cols] = (y_own[:, cols] + (y_oth[:, cols] + part)).astype(BF16)
        copy = pltpu.make_async_copy(y_out.at[:, cols], y_hbm.at[:, cols], out_sem.at[c])
        copy.start()
        copies.append(copy)
    for copy in copies:
        copy.wait()


def solution(mesh):
    n_blocks = mesh.shape['cp']

    def layer(x_loc, seg_loc, w_query, w_key, w_value, w_out):
        chunk, width = x_loc.shape
        kv_heads = w_key.shape[1] // HEAD
        heads = w_query.shape[1] // HEAD
        pieces = 3
        dma = pltpu.SemaphoreType.DMA
        any_spec = pl.BlockSpec(memory_space=pl.ANY)
        vmem_spec = pl.BlockSpec(memory_space=pltpu.VMEM)
        parts = pl.pallas_call(
            layer_kernel,
            out_shape=(
                pltpu.VMEM((chunk, width), F32),
                pltpu.VMEM((chunk, width), F32),
                pltpu.VMEM((heads, chunk, HEAD), BF16),
                pltpu.VMEM(w_out.shape, BF16),
            ),
            in_specs=[any_spec] * 6,
            out_specs=[vmem_spec] * 4,
            scratch_shapes=[
                pltpu.VMEM((n_blocks, 1, chunk), jnp.int32),
                pltpu.VMEM((chunk, HEAD), jnp.int32),
                pltpu.VMEM((chunk, width), BF16),
                pltpu.VMEM((4, width, TILE), BF16),
                pltpu.VMEM((2 * kv_heads, n_blocks * chunk, HEAD), BF16),
                pltpu.VMEM((heads, chunk, HEAD), BF16),
                pltpu.VMEM((heads, chunk, HEAD), BF16),
                pltpu.VMEM(w_out.shape, BF16),
                pltpu.SemaphoreType.REGULAR, dma((3,)), dma((4,)),
                dma((3,)), dma((3,)), dma((3,)), dma((3,)),
                dma((pieces,)), dma((pieces,)), dma((pieces,)), dma((pieces,)),
                dma((pieces,)), dma((pieces,)), dma((pieces,)), dma((pieces,)),
                dma((len(SENDS),)), dma((len(SENDS),)),
            ],
            compiler_params=pltpu.CompilerParams(collective_id=0, has_side_effects=True, vmem_limit_bytes=36 * 2 ** 20),
        )(seg_loc.reshape(1, chunk), x_loc, w_query, w_key, w_value, w_out)
        parts = [pltpu.with_memory_space_constraint(a, pltpu.VMEM) for a in parts]

        def last_head(me):
            return (3 - me) * (heads // kv_heads) + heads // kv_heads - 1

        return pl.pallas_call(
            functools.partial(last_kernel, last_head),
            out_shape=jax.ShapeDtypeStruct((chunk, width), BF16),
            in_specs=[vmem_spec] * 4,
            out_specs=any_spec,
            scratch_shapes=[pltpu.VMEM((chunk, width), BF16), dma((width // COLS,))],
            compiler_params=pltpu.CompilerParams(vmem_limit_bytes=8 * 2 ** 20),
        )(*parts)

    rows = P(('dp', 'cp'), None)
    return jax.shard_map(layer, mesh=mesh,
                         in_specs=(rows, P(('dp', 'cp')), P(None, 'tp'), P(None, 'tp'), P(None, 'tp'), P('tp', None)),
                         out_specs=rows, check_vma=False)
```

```python
import functools
import math

import jax
import jax.numpy as jnp
from jax import lax
from jax.experimental import pallas as pl
from jax.experimental.pallas import tpu as pltpu
from jax.sharding import PartitionSpec as P

HEAD = 128
TILE = 256
COLS = 512
EXTRA = 8
SENDS = ((0, 3), (3, 3), (6, 2), (8, 2), (10, 1), (11, 1))
MESH = pl.DeviceIdType.MESH
F32 = jnp.float32
BF16 = jnp.bfloat16
SCALE = HEAD ** -0.5 * math.log2(math.e)


def layer_kernel(seg_hbm, x_hbm, wq_hbm, wk_hbm, wv_hbm, wo_hbm,
                 y_own, y_oth, o_oth, w_oth,
                 seg, segq, xbuf, wbuf, kv, q, o_own, wo,
                 entry, load_sem, tile_sem, seg_s, seg_r, kv_s, kv_r,
                 y_s, y_r, xf_s, xf_r, d1_s, d1_r, d2_s, d2_r, o_s, o_r):
    chunk, width = xbuf.shape
    kv_heads = kv.shape[0] // 2
    heads = q.shape[0]
    group = heads // kv_heads
    n_blocks = seg.shape[0]
    quarter = wo.shape[0] // n_blocks
    pieces = y_s.shape[0]
    piece = quarter // pieces
    n_cols = width // COLS
    kv_tiles = 2 * kv_heads * HEAD // TILE
    q_tiles = heads * HEAD // TILE
    slots = wbuf.shape[0]

    dp = lax.axis_index('dp')
    tp = lax.axis_index('tp')
    me = lax.axis_index('cp')
    core_peer = me + 1 - 2 * lax.rem(me, 2)
    chip_peer = lax.rem(me + 2, 4)
    far_peer = 3 - me
    others = (core_peer, chip_peer, far_peer)
    tp_peer = (dp, 1 - tp, me)

    def at(block):
        return (dp, tp, block)

    def remote(src, dst, s_sem, r_sem, where):
        return pltpu.make_async_remote_copy(src_ref=src, dst_ref=dst, send_sem=s_sem, recv_sem=r_sem,
                                            device_id=where, device_id_type=MESH)

    odd = lax.rem(me, 2)
    barrier = pltpu.get_barrier_semaphore()
    for where in (tp_peer, at(core_peer)):
        pl.semaphore_signal(barrier, inc=1, device_id=where, device_id_type=MESH)

    @pl.when(odd == 1)
    def _():
        pl.semaphore_signal(barrier, inc=1, device_id=at(chip_peer), device_id_type=MESH)

    def kv_tile_src(t):
        per = kv_tiles // 2
        return (wk_hbm if t < per else wv_hbm).at[:, pl.ds((t % per) * TILE, TILE)]

    def tile_copy(src, slot):
        return pltpu.make_async_copy(src, wbuf.at[slot], tile_sem.at[slot])

    def q_tile_src(t):
        return wq_hbm.at[:, pl.ds(pl.multiple_of(t * TILE, TILE), TILE)]

    x_load = pltpu.make_async_copy(x_hbm, xbuf, load_sem.at[0])
    wo_load = pltpu.make_async_copy(wo_hbm, wo, load_sem.at[2])
    seg_load = pltpu.make_async_copy(seg_hbm, seg.at[me], load_sem.at[1])

    x_load.start()
    for t in range(kv_tiles):
        tile_copy(kv_tile_src(t), t).start()
    seg_load.start()


    def rows_of(block, i, moved):
        begin = -EXTRA if moved and i == 0 else 0
        end = -EXTRA if moved and i == pieces - 1 else 0
        return pl.ds(pl.multiple_of(block * quarter + i * piece + begin, 8), piece - begin + end)

    def by_piece(block, i, side, act):
        if 0 < i < pieces - 1:
            act(False)
            return
        edge = ((block == 2) if i == 0 else (block == 1)) & (side == 0)
        for moved in (False, True):
            @pl.when(edge if moved else jnp.logical_not(edge))
            def _(moved=moved):
                act(moved)

    def y_copy(i, moved):
        rows = rows_of(me, i, moved)
        return remote(wo_hbm.at[rows], w_oth.at[rows], y_s.at[i], y_r.at[i], tp_peer)

    def hand_on(block, i, moved, s_sem, r_sem, where):
        part = w_oth.at[rows_of(block, i, moved)]
        return remote(part, part, s_sem.at[i], r_sem.at[i], where)

    def seg_copy(k, block, where):
        return remote(seg.at[block], seg.at[block], seg_s.at[k], seg_r.at[k], where)

    def kv_copy(k, block, where):
        part = kv.at[:, pl.ds(pl.multiple_of(block * chunk, chunk), chunk), :]
        return remote(part, part, kv_s.at[k], kv_r.at[k], where)

    def o_copy(k):
        part = pl.ds(*SENDS[k])
        return remote(o_own.at[part], o_oth.at[part], o_s.at[k], o_r.at[k], tp_peer)

    def group_of(j):
        high = lax.rem(me // 2 + j // 2, 2)
        low = lax.rem(lax.rem(me, 2) + lax.rem(j, 2), 2)
        return 2 * high + low

    def place_of(u):
        half = u // 6
        v = u - 6 * half
        end = v // 4
        j = (1 - half) * (v // 3) + half * (2 + (1 - end) * (v // 2) + end * (v - 4))
        i = (1 - half) * (v % 3) + half * ((1 - end) * (v % 2) + 2 * end)
        return j, i

    def head_of(u):
        j, i = place_of(u)
        return group_of(j) * group + i

    pl.semaphore_wait(barrier, 2 + odd)
    for i in range(pieces):
        by_piece(me, i, 1 - tp, lambda moved, i=i: y_copy(i, moved).start())

    @pl.when(odd == 1)
    def _():
        pl.semaphore_signal(entry, inc=1, device_id=at(chip_peer), device_id_type=MESH)
        pl.semaphore_wait(entry, 1)
        pl.semaphore_signal(entry, inc=1, device_id=at(core_peer), device_id_type=MESH)

    @pl.when(odd == 0)
    def _():
        pl.semaphore_wait(entry, 1)

    seg_load.wait()
    for k, block in enumerate(others):
        seg_copy(k, me, at(block)).start()

    x_load.wait()
    own_rows = pl.ds(pl.multiple_of(me * chunk, chunk), chunk)

    def project_kv(t, _):
        tile_copy(wk_hbm.at[:, pl.ds(0, TILE)], t).wait()
        part = jnp.dot(xbuf[...], wbuf[t], preferred_element_type=F32).astype(BF16)
        for k in range(TILE // HEAD):
            kv[t * (TILE // HEAD) + k, own_rows, :] = part[:, k * HEAD:(k + 1) * HEAD]

        @pl.when(t < q_tiles)
        def _():
            tile_copy(q_tile_src(t), t).start()
        return 0

    lax.fori_loop(0, kv_tiles, project_kv, 0)

    def project_q(t, _):
        slot = lax.rem(t, slots)
        tile_copy(q_tile_src(t), slot).wait()
        part = jnp.dot(xbuf[...], wbuf[slot], preferred_element_type=F32).astype(BF16)
        for k in range(TILE // HEAD):
            q[t * (TILE // HEAD) + k] = part[:, k * HEAD:(k + 1) * HEAD]

        @pl.when(t + slots < q_tiles)
        def _():
            tile_copy(q_tile_src(t + slots), slot).start()

        @pl.when(t == 0)
        def _():
            @pl.when(me < 2)
            def _():
                kv_copy(0, me, at(chip_peer)).start()
            kv_copy(1, me, at(core_peer)).start()
            wo_load.start()
        return 0

    lax.fori_loop(0, q_tiles, project_q, 0)

    def pass_y(i):
        def act(moved):
            y_copy(i, moved).wait_recv()
            hand_on(me, i, moved, xf_s, xf_r, at(chip_peer)).start()
            hand_on(me, i, moved, d1_s, d1_r, at(core_peer)).start()
        by_piece(me, i, tp, act)

    def pass_x(i):
        def act(moved):
            hand_on(chip_peer, i, moved, xf_s, xf_r, at(chip_peer)).wait_recv()
            hand_on(chip_peer, i, moved, d2_s, d2_r, at(core_peer)).start()
        by_piece(chip_peer, i, tp, act)

    def wait_near(i):
        by_piece(core_peer, i, tp, lambda moved: hand_on(core_peer, i, moved, d1_s, d1_r, at(core_peer)).wait_recv())

    def wait_far(i):
        by_piece(far_peer, i, tp, lambda moved: hand_on(far_peer, i, moved, d2_s, d2_r, at(core_peer)).wait_recv())

    pass_y(0)
    for k, block in enumerate(others):
        seg_copy(k, block, at(block)).wait_recv()
    seg_col = jnp.transpose(jnp.broadcast_to(seg[me], (HEAD, chunk)))
    segq[...] = seg_col

    kv_copy(1, core_peer, at(core_peer)).wait_recv()

    @pl.when(me >= 2)
    def _():
        kv_copy(0, chip_peer, at(chip_peer)).wait_recv()
        kv_copy(2, chip_peer, at(core_peer)).start()
        kv_copy(2, far_peer, at(core_peer)).wait_recv()

    def attend(u, h, g, r, n):
        rows = pl.ds(pl.multiple_of(r * TILE, TILE), TILE)
        q_t = q[h, rows, :]
        sq = segq[rows, :]
        sq = jnp.concatenate([sq] * (chunk // HEAD), axis=1)
        parts = []
        for b in range(n):
            s = lax.dot_general(q_t, kv[g, pl.ds(b * chunk, chunk), :], (((1,), (1,)), ((), ())), preferred_element_type=F32)
            ok = sq == seg[b]
            if b == n - 1:
                q_pos = r * TILE + lax.broadcasted_iota(jnp.int32, (TILE, chunk), 0)
                ok = ok & (q_pos >= lax.broadcasted_iota(jnp.int32, (TILE, chunk), 1))
            parts.append(jnp.where(ok, s, -jnp.inf))
        top = parts[0].max(axis=1, keepdims=True)
        for s in parts[1:]:
            top = jnp.maximum(top, s.max(axis=1, keepdims=True))
        total = None
        acc = None
        for b, s in enumerate(parts):
            p = jnp.exp2((s - top) * SCALE)
            row_sum = p.sum(axis=1, keepdims=True)
            pv = jnp.dot(p.astype(BF16), kv[kv_heads + g, pl.ds(b * chunk, chunk), :], preferred_element_type=F32)
            total = row_sum if total is None else total + row_sum
            acc = pv if acc is None else acc + pv
        o_own[u, rows, :] = (acc / total).astype(BF16)

    def attend_head(u, _):
        h = head_of(u)
        g = h // group
        for n in range(1, n_blocks + 1):
            @pl.when(me == n - 1)
            def _(n=n):
                def one(r, c):
                    attend(u, h, g, r, n)
                    return c
                lax.fori_loop(0, chunk // TILE, one, 0)

        for k, (begin, count) in enumerate(SENDS[:-1]):
            @pl.when(u == begin + count)
            def _(k=k):
                o_copy(k).start()

        @pl.when(u == group - 1)
        def _():
            pass_y(1)

        @pl.when(u == 3 * group - 1)
        def _():
            pass_x(0)
        return 0

    lax.fori_loop(0, heads, attend_head, 0)
    pass_y(2)

    def add_rows(o_ref, w_ref, y_ref, u, count, first):
        rows = pl.ds(pl.multiple_of(head_of(u) * HEAD, HEAD), count * HEAD)

        def one(c, carry):
            cols = pl.ds(pl.multiple_of(c * COLS, COLS), COLS)
            left = jnp.concatenate([o_ref[u + k] for k in range(count)], axis=1)
            part = jnp.dot(left, w_ref[rows, cols], preferred_element_type=F32)
            y_ref[:, cols] = part if first else y_ref[:, cols] + part
            return carry

        lax.fori_loop(0, n_cols, one, 0)

    wo_load.wait()
    runs = ((0, 3), (3, 3), (6, 2), (8, 2), (10, 1))
    for u, count in runs:
        add_rows(o_own, wo, y_own, u, count, u == 0)
        if u == 0:
            o_copy(len(SENDS) - 1).start()
    add_rows(o_own, wo, y_own, heads - 1, 1, False)

    pass_x(1)
    for u, count in runs:
        for k, (begin, _) in enumerate(SENDS):
            if u <= begin < u + count:
                o_copy(k).wait_recv()
        if u == 0:
            wait_far(0)
        if u == 3:
            for i in range(pieces):
                wait_near(i)
        if u == 8:
            for i in range(1, pieces - 1):
                wait_far(i)
        if u == 10:
            pass_x(2)
        add_rows(o_oth, w_oth, y_oth, u, count, u == 0)
    wait_far(pieces - 1)

    o_copy(len(SENDS) - 1).wait_recv()

    for i in range(pieces):
        def sent(moved, i=i):
            hand_on(me, i, moved, xf_s, xf_r, at(chip_peer)).wait_send()
            hand_on(me, i, moved, d1_s, d1_r, at(core_peer)).wait_send()
        by_piece(me, i, 1 - tp, lambda moved, i=i: y_copy(i, moved).wait_send())
        by_piece(me, i, tp, sent)
        by_piece(chip_peer, i, tp, lambda moved, i=i: hand_on(chip_peer, i, moved, d2_s, d2_r, at(core_peer)).wait_send())
    for k, block in enumerate(others):
        seg_copy(k, me, at(block)).wait_send()
    kv_copy(1, me, at(core_peer)).wait_send()

    @pl.when(me < 2)
    def _():
        kv_copy(0, me, at(chip_peer)).wait_send()

    @pl.when(me >= 2)
    def _():
        kv_copy(2, chip_peer, at(core_peer)).wait_send()

    for k in range(len(SENDS)):
        o_copy(k).wait_send()


def last_kernel(last_head, y_own, y_oth, o_oth, w_oth, y_hbm, y_out, out_sem):
    h = last_head(lax.axis_index('cp'))
    left = o_oth[o_oth.shape[0] - 1]
    rows = pl.ds(pl.multiple_of(h * HEAD, HEAD), HEAD)
    copies = []
    for c in range(y_out.shape[1] // COLS):
        cols = pl.ds(c * COLS, COLS)
        part = jnp.dot(left, w_oth[rows, cols], preferred_element_type=F32)
        y_out[:, cols] = (y_own[:, cols] + (y_oth[:, cols] + part)).astype(BF16)
        copy = pltpu.make_async_copy(y_out.at[:, cols], y_hbm.at[:, cols], out_sem.at[c])
        copy.start()
        copies.append(copy)
    for copy in copies:
        copy.wait()


def solution(mesh):
    n_blocks = mesh.shape['cp']

    def layer(x_loc, seg_loc, w_query, w_key, w_value, w_out):
        chunk, width = x_loc.shape
        kv_heads = w_key.shape[1] // HEAD
        heads = w_query.shape[1] // HEAD
        pieces = 3
        dma = pltpu.SemaphoreType.DMA
        any_spec = pl.BlockSpec(memory_space=pl.ANY)
        vmem_spec = pl.BlockSpec(memory_space=pltpu.VMEM)
        parts = pl.pallas_call(
            layer_kernel,
            out_shape=(
                pltpu.VMEM((chunk, width), F32),
                pltpu.VMEM((chunk, width), F32),
                pltpu.VMEM((heads, chunk, HEAD), BF16),
                pltpu.VMEM(w_out.shape, BF16),
            ),
            in_specs=[any_spec] * 6,
            out_specs=[vmem_spec] * 4,
            scratch_shapes=[
                pltpu.VMEM((n_blocks, 1, chunk), jnp.int32),
                pltpu.VMEM((chunk, HEAD), jnp.int32),
                pltpu.VMEM((chunk, width), BF16),
                pltpu.VMEM((4, width, TILE), BF16),
                pltpu.VMEM((2 * kv_heads, n_blocks * chunk, HEAD), BF16),
                pltpu.VMEM((heads, chunk, HEAD), BF16),
                pltpu.VMEM((heads, chunk, HEAD), BF16),
                pltpu.VMEM(w_out.shape, BF16),
                pltpu.SemaphoreType.REGULAR, dma((3,)), dma((4,)),
                dma((3,)), dma((3,)), dma((3,)), dma((3,)),
                dma((pieces,)), dma((pieces,)), dma((pieces,)), dma((pieces,)),
                dma((pieces,)), dma((pieces,)), dma((pieces,)), dma((pieces,)),
                dma((len(SENDS),)), dma((len(SENDS),)),
            ],
            compiler_params=pltpu.CompilerParams(collective_id=0, has_side_effects=True, vmem_limit_bytes=36 * 2 ** 20),
        )(seg_loc.reshape(1, chunk), x_loc, w_query, w_key, w_value, w_out)
        parts = [pltpu.with_memory_space_constraint(a, pltpu.VMEM) for a in parts]

        def last_head(me):
            return (3 - me) * (heads // kv_heads) + heads // kv_heads - 1

        return pl.pallas_call(
            functools.partial(last_kernel, last_head),
            out_shape=jax.ShapeDtypeStruct((chunk, width), BF16),
            in_specs=[vmem_spec] * 4,
            out_specs=any_spec,
            scratch_shapes=[pltpu.VMEM((chunk, width), BF16), dma((width // COLS,))],
            compiler_params=pltpu.CompilerParams(vmem_limit_bytes=8 * 2 ** 20),
        )(*parts)

    rows = P(('dp', 'cp'), None)
    return jax.shard_map(layer, mesh=mesh,
                         in_specs=(rows, P(('dp', 'cp')), P(None, 'tp'), P(None, 'tp'), P(None, 'tp'), P('tp', None)),
                         out_specs=rows, check_vma=False)
```

```python
import functools
import math

import jax
import jax.numpy as jnp
from jax import lax
from jax.experimental import pallas as pl
from jax.experimental.pallas import tpu as pltpu
from jax.sharding import PartitionSpec as P

HEAD = 128
TILE = 256
COLS = 512
EXTRA = 16
EARLY = (2, 3)
SHORT = (1, 2)
SENDS = ((0, 3), (3, 3), (6, 2), (8, 2), (10, 1), (11, 1))
MESH = pl.DeviceIdType.MESH
F32 = jnp.float32
BF16 = jnp.bfloat16
SCALE = HEAD ** -0.5 * math.log2(math.e)


def layer_kernel(seg_hbm, x_hbm, wq_hbm, wk_hbm, wv_hbm, wo_hbm,
                 y_own, y_oth, o_oth, w_oth,
                 seg, segq, xbuf, wbuf, kv, q, o_own, wo,
                 entry, load_sem, tile_sem, seg_s, seg_r, kv_s, kv_r,
                 y_s, y_r, xf_s, xf_r, d1_s, d1_r, d2_s, d2_r, o_s, o_r):
    chunk, width = xbuf.shape
    kv_heads = kv.shape[0] // 2
    heads = q.shape[0]
    group = heads // kv_heads
    n_blocks = seg.shape[0]
    quarter = wo.shape[0] // n_blocks
    pieces = y_s.shape[0]
    piece = quarter // pieces
    n_cols = width // COLS
    kv_tiles = 2 * kv_heads * HEAD // TILE
    q_tiles = heads * HEAD // TILE
    slots = wbuf.shape[0]

    dp = lax.axis_index('dp')
    tp = lax.axis_index('tp')
    me = lax.axis_index('cp')
    core_peer = me + 1 - 2 * lax.rem(me, 2)
    chip_peer = lax.rem(me + 2, 4)
    far_peer = 3 - me
    others = (core_peer, chip_peer, far_peer)
    tp_peer = (dp, 1 - tp, me)

    def at(block):
        return (dp, tp, block)

    def remote(src, dst, s_sem, r_sem, where):
        return pltpu.make_async_remote_copy(src_ref=src, dst_ref=dst, send_sem=s_sem, recv_sem=r_sem,
                                            device_id=where, device_id_type=MESH)

    odd = lax.rem(me, 2)
    barrier = pltpu.get_barrier_semaphore()
    for where in (tp_peer, at(core_peer)):
        pl.semaphore_signal(barrier, inc=1, device_id=where, device_id_type=MESH)

    @pl.when(odd == 1)
    def _():
        pl.semaphore_signal(barrier, inc=1, device_id=at(chip_peer), device_id_type=MESH)

    def kv_tile_src(t):
        per = kv_tiles // 2
        return (wk_hbm if t < per else wv_hbm).at[:, pl.ds((t % per) * TILE, TILE)]

    def tile_copy(src, slot):
        return pltpu.make_async_copy(src, wbuf.at[slot], tile_sem.at[slot])

    def q_tile_src(t):
        return wq_hbm.at[:, pl.ds(pl.multiple_of(t * TILE, TILE), TILE)]

    x_load = pltpu.make_async_copy(x_hbm, xbuf, load_sem.at[0])
    wo_load = pltpu.make_async_copy(wo_hbm, wo, load_sem.at[2])
    seg_load = pltpu.make_async_copy(seg_hbm, seg.at[me], load_sem.at[1])

    x_load.start()
    for t in range(kv_tiles):
        tile_copy(kv_tile_src(t), t).start()
    seg_load.start()


    def rows_of(block, i, moved):
        begin = -EXTRA if moved and i == 0 else 0
        end = -EXTRA if moved and i == pieces - 1 else 0
        return pl.ds(pl.multiple_of(block * quarter + i * piece + begin, 8), piece - begin + end)

    def by_piece(block, i, side, act):
        if 0 < i < pieces - 1:
            act(False)
            return
        low, high = EARLY if i == 0 else SHORT
        edge = (block >= low) & (block <= high) & (side == 0)
        for moved in (False, True):
            @pl.when(edge if moved else jnp.logical_not(edge))
            def _(moved=moved):
                act(moved)

    def y_copy(i, moved):
        rows = rows_of(me, i, moved)
        return remote(wo_hbm.at[rows], w_oth.at[rows], y_s.at[i], y_r.at[i], tp_peer)

    def hand_on(block, i, moved, s_sem, r_sem, where):
        part = w_oth.at[rows_of(block, i, moved)]
        return remote(part, part, s_sem.at[i], r_sem.at[i], where)

    def seg_copy(k, block, where):
        return remote(seg.at[block], seg.at[block], seg_s.at[k], seg_r.at[k], where)

    def kv_copy(k, block, where):
        part = kv.at[:, pl.ds(pl.multiple_of(block * chunk, chunk), chunk), :]
        return remote(part, part, kv_s.at[k], kv_r.at[k], where)

    def o_copy(k):
        part = pl.ds(*SENDS[k])
        return remote(o_own.at[part], o_oth.at[part], o_s.at[k], o_r.at[k], tp_peer)

    def group_of(j):
        high = lax.rem(me // 2 + j // 2, 2)
        low = lax.rem(lax.rem(me, 2) + lax.rem(j, 2), 2)
        return 2 * high + low

    def place_of(u):
        half = u // 6
        v = u - 6 * half
        end = v // 4
        j = (1 - half) * (v // 3) + half * (2 + (1 - end) * (v // 2) + end * (v - 4))
        i = (1 - half) * (v % 3) + half * ((1 - end) * (v % 2) + 2 * end)
        return j, i

    def head_of(u):
        j, i = place_of(u)
        return group_of(j) * group + i

    pl.semaphore_wait(barrier, 2 + odd)
    for i in range(pieces):
        by_piece(me, i, 1 - tp, lambda moved, i=i: y_copy(i, moved).start())

    @pl.when(odd == 1)
    def _():
        pl.semaphore_signal(entry, inc=1, device_id=at(chip_peer), device_id_type=MESH)
        pl.semaphore_wait(entry, 1)
        pl.semaphore_signal(entry, inc=1, device_id=at(core_peer), device_id_type=MESH)

    @pl.when(odd == 0)
    def _():
        pl.semaphore_wait(entry, 1)

    seg_load.wait()
    for k, block in enumerate(others):
        seg_copy(k, me, at(block)).start()

    x_load.wait()
    own_rows = pl.ds(pl.multiple_of(me * chunk, chunk), chunk)

    def project_kv(t, _):
        tile_copy(wk_hbm.at[:, pl.ds(0, TILE)], t).wait()
        part = jnp.dot(xbuf[...], wbuf[t], preferred_element_type=F32).astype(BF16)
        for k in range(TILE // HEAD):
            kv[t * (TILE // HEAD) + k, own_rows, :] = part[:, k * HEAD:(k + 1) * HEAD]

        @pl.when(t < q_tiles)
        def _():
            tile_copy(q_tile_src(t), t).start()
        return 0

    lax.fori_loop(0, kv_tiles, project_kv, 0)

    def project_q(t, _):
        slot = lax.rem(t, slots)
        tile_copy(q_tile_src(t), slot).wait()
        part = jnp.dot(xbuf[...], wbuf[slot], preferred_element_type=F32).astype(BF16)
        for k in range(TILE // HEAD):
            q[t * (TILE // HEAD) + k] = part[:, k * HEAD:(k + 1) * HEAD]

        @pl.when(t + slots < q_tiles)
        def _():
            tile_copy(q_tile_src(t + slots), slot).start()

        @pl.when(t == 0)
        def _():
            @pl.when(me < 2)
            def _():
                kv_copy(0, me, at(chip_peer)).start()
            kv_copy(1, me, at(core_peer)).start()
            wo_load.start()
        return 0

    lax.fori_loop(0, q_tiles, project_q, 0)

    def pass_y(i):
        def act(moved):
            y_copy(i, moved).wait_recv()
            hand_on(me, i, moved, xf_s, xf_r, at(chip_peer)).start()
            hand_on(me, i, moved, d1_s, d1_r, at(core_peer)).start()
        by_piece(me, i, tp, act)

    def pass_x(i):
        def act(moved):
            hand_on(chip_peer, i, moved, xf_s, xf_r, at(chip_peer)).wait_recv()
            hand_on(chip_peer, i, moved, d2_s, d2_r, at(core_peer)).start()
        by_piece(chip_peer, i, tp, act)

    def wait_near(i):
        by_piece(core_peer, i, tp, lambda moved: hand_on(core_peer, i, moved, d1_s, d1_r, at(core_peer)).wait_recv())

    def wait_far(i):
        by_piece(far_peer, i, tp, lambda moved: hand_on(far_peer, i, moved, d2_s, d2_r, at(core_peer)).wait_recv())

    pass_y(0)
    for k, block in enumerate(others):
        seg_copy(k, block, at(block)).wait_recv()
    seg_col = jnp.transpose(jnp.broadcast_to(seg[me], (HEAD, chunk)))
    segq[...] = seg_col

    kv_copy(1, core_peer, at(core_peer)).wait_recv()

    @pl.when(me >= 2)
    def _():
        kv_copy(0, chip_peer, at(chip_peer)).wait_recv()
        kv_copy(2, chip_peer, at(core_peer)).start()
        kv_copy(2, far_peer, at(core_peer)).wait_recv()

    def attend(u, h, g, r, n):
        rows = pl.ds(pl.multiple_of(r * TILE, TILE), TILE)
        q_t = q[h, rows, :]
        sq = segq[rows, :]
        sq = jnp.concatenate([sq] * (chunk // HEAD), axis=1)
        parts = []
        for b in range(n):
            s = lax.dot_general(q_t, kv[g, pl.ds(b * chunk, chunk), :], (((1,), (1,)), ((), ())), preferred_element_type=F32)
            ok = sq == seg[b]
            if b == n - 1:
                q_pos = r * TILE + lax.broadcasted_iota(jnp.int32, (TILE, chunk), 0)
                ok = ok & (q_pos >= lax.broadcasted_iota(jnp.int32, (TILE, chunk), 1))
            parts.append(jnp.where(ok, s, -jnp.inf))
        top = parts[0].max(axis=1, keepdims=True)
        for s in parts[1:]:
            top = jnp.maximum(top, s.max(axis=1, keepdims=True))
        total = None
        acc = None
        for b, s in enumerate(parts):
            p = jnp.exp2((s - top) * SCALE)
            row_sum = p.sum(axis=1, keepdims=True)
            pv = jnp.dot(p.astype(BF16), kv[kv_heads + g, pl.ds(b * chunk, chunk), :], preferred_element_type=F32)
            total = row_sum if total is None else total + row_sum
            acc = pv if acc is None else acc + pv
        o_own[u, rows, :] = (acc / total).astype(BF16)

    def attend_head(u, _):
        h = head_of(u)
        g = h // group
        for n in range(1, n_blocks + 1):
            @pl.when(me == n - 1)
            def _(n=n):
                def one(r, c):
                    attend(u, h, g, r, n)
                    return c
                lax.fori_loop(0, chunk // TILE, one, 0)

        for k, (begin, count) in enumerate(SENDS[:-1]):
            @pl.when(u == begin + count)
            def _(k=k):
                o_copy(k).start()

        @pl.when(u == group - 1)
        def _():
            pass_y(1)

        @pl.when(u == 3 * group - 1)
        def _():
            pass_x(0)
        return 0

    lax.fori_loop(0, heads, attend_head, 0)
    pass_y(2)

    def add_rows(o_ref, w_ref, y_ref, u, count, first):
        rows = pl.ds(pl.multiple_of(head_of(u) * HEAD, HEAD), count * HEAD)

        def one(c, carry):
            cols = pl.ds(pl.multiple_of(c * COLS, COLS), COLS)
            left = jnp.concatenate([o_ref[u + k] for k in range(count)], axis=1)
            part = jnp.dot(left, w_ref[rows, cols], preferred_element_type=F32)
            y_ref[:, cols] = part if first else y_ref[:, cols] + part
            return carry

        lax.fori_loop(0, n_cols, one, 0)

    wo_load.wait()
    runs = ((0, 3), (3, 3), (6, 2), (8, 2), (10, 1))
    for u, count in runs:
        add_rows(o_own, wo, y_own, u, count, u == 0)
        if u == 0:
            o_copy(len(SENDS) - 1).start()
    add_rows(o_own, wo, y_own, heads - 1, 1, False)

    pass_x(1)
    for u, count in runs:
        for k, (begin, _) in enumerate(SENDS):
            if u <= begin < u + count:
                o_copy(k).wait_recv()
        if u == 0:
            wait_near(0)
            wait_far(0)
        if u == 3:
            for i in range(1, pieces):
                wait_near(i)
        if u == 8:
            for i in range(1, pieces - 1):
                wait_far(i)
        if u == 10:
            pass_x(2)
        add_rows(o_oth, w_oth, y_oth, u, count, u == 0)
    wait_far(pieces - 1)

    o_copy(len(SENDS) - 1).wait_recv()

    for i in range(pieces):
        def sent(moved, i=i):
            hand_on(me, i, moved, xf_s, xf_r, at(chip_peer)).wait_send()
            hand_on(me, i, moved, d1_s, d1_r, at(core_peer)).wait_send()
        by_piece(me, i, 1 - tp, lambda moved, i=i: y_copy(i, moved).wait_send())
        by_piece(me, i, tp, sent)
        by_piece(chip_peer, i, tp, lambda moved, i=i: hand_on(chip_peer, i, moved, d2_s, d2_r, at(core_peer)).wait_send())
    for k, block in enumerate(others):
        seg_copy(k, me, at(block)).wait_send()
    kv_copy(1, me, at(core_peer)).wait_send()

    @pl.when(me < 2)
    def _():
        kv_copy(0, me, at(chip_peer)).wait_send()

    @pl.when(me >= 2)
    def _():
        kv_copy(2, chip_peer, at(core_peer)).wait_send()

    for k in range(len(SENDS)):
        o_copy(k).wait_send()


def last_kernel(last_head, y_own, y_oth, o_oth, w_oth, y_hbm, y_out, out_sem):
    h = last_head(lax.axis_index('cp'))
    left = o_oth[o_oth.shape[0] - 1]
    rows = pl.ds(pl.multiple_of(h * HEAD, HEAD), HEAD)
    copies = []
    for c in range(y_out.shape[1] // COLS):
        cols = pl.ds(c * COLS, COLS)
        part = jnp.dot(left, w_oth[rows, cols], preferred_element_type=F32)
        y_out[:, cols] = (y_own[:, cols] + (y_oth[:, cols] + part)).astype(BF16)
        copy = pltpu.make_async_copy(y_out.at[:, cols], y_hbm.at[:, cols], out_sem.at[c])
        copy.start()
        copies.append(copy)
    for copy in copies:
        copy.wait()


def solution(mesh):
    n_blocks = mesh.shape['cp']

    def layer(x_loc, seg_loc, w_query, w_key, w_value, w_out):
        chunk, width = x_loc.shape
        kv_heads = w_key.shape[1] // HEAD
        heads = w_query.shape[1] // HEAD
        pieces = 3
        dma = pltpu.SemaphoreType.DMA
        any_spec = pl.BlockSpec(memory_space=pl.ANY)
        vmem_spec = pl.BlockSpec(memory_space=pltpu.VMEM)
        parts = pl.pallas_call(
            layer_kernel,
            out_shape=(
                pltpu.VMEM((chunk, width), F32),
                pltpu.VMEM((chunk, width), F32),
                pltpu.VMEM((heads, chunk, HEAD), BF16),
                pltpu.VMEM(w_out.shape, BF16),
            ),
            in_specs=[any_spec] * 6,
            out_specs=[vmem_spec] * 4,
            scratch_shapes=[
                pltpu.VMEM((n_blocks, 1, chunk), jnp.int32),
                pltpu.VMEM((chunk, HEAD), jnp.int32),
                pltpu.VMEM((chunk, width), BF16),
                pltpu.VMEM((4, width, TILE), BF16),
                pltpu.VMEM((2 * kv_heads, n_blocks * chunk, HEAD), BF16),
                pltpu.VMEM((heads, chunk, HEAD), BF16),
                pltpu.VMEM((heads, chunk, HEAD), BF16),
                pltpu.VMEM(w_out.shape, BF16),
                pltpu.SemaphoreType.REGULAR, dma((3,)), dma((4,)),
                dma((3,)), dma((3,)), dma((3,)), dma((3,)),
                dma((pieces,)), dma((pieces,)), dma((pieces,)), dma((pieces,)),
                dma((pieces,)), dma((pieces,)), dma((pieces,)), dma((pieces,)),
                dma((len(SENDS),)), dma((len(SENDS),)),
            ],
            compiler_params=pltpu.CompilerParams(collective_id=0, has_side_effects=True, vmem_limit_bytes=36 * 2 ** 20),
        )(seg_loc.reshape(1, chunk), x_loc, w_query, w_key, w_value, w_out)
        parts = [pltpu.with_memory_space_constraint(a, pltpu.VMEM) for a in parts]

        def last_head(me):
            return (3 - me) * (heads // kv_heads) + heads // kv_heads - 1

        return pl.pallas_call(
            functools.partial(last_kernel, last_head),
            out_shape=jax.ShapeDtypeStruct((chunk, width), BF16),
            in_specs=[vmem_spec] * 4,
            out_specs=any_spec,
            scratch_shapes=[pltpu.VMEM((chunk, width), BF16), dma((width // COLS,))],
            compiler_params=pltpu.CompilerParams(vmem_limit_bytes=8 * 2 ** 20),
        )(*parts)

    rows = P(('dp', 'cp'), None)
    return jax.shard_map(layer, mesh=mesh,
                         in_specs=(rows, P(('dp', 'cp')), P(None, 'tp'), P(None, 'tp'), P(None, 'tp'), P('tp', None)),
                         out_specs=rows, check_vma=False)
```

```python
import functools
import math

import jax
import jax.numpy as jnp
from jax import lax
from jax.experimental import pallas as pl
from jax.experimental.pallas import tpu as pltpu
from jax.sharding import PartitionSpec as P

HEAD = 128
TILE = 256
COLS = 512
EXTRA = 16
EARLY = (2, 3)
SHORT = (1, 2)
SENDS = ((0, 3), (3, 3), (6, 2), (8, 2), (10, 1), (11, 1))
MESH = pl.DeviceIdType.MESH
F32 = jnp.float32
BF16 = jnp.bfloat16
SCALE = HEAD ** -0.5 * math.log2(math.e)


def layer_kernel(seg_hbm, x_hbm, wq_hbm, wk_hbm, wv_hbm, wo_hbm,
                 y_own, y_oth, o_oth, w_oth,
                 seg, segq, xbuf, wbuf, kv, q, o_own, wo,
                 entry, load_sem, tile_sem, seg_s, seg_r, kv_s, kv_r,
                 y_s, y_r, xf_s, xf_r, d1_s, d1_r, d2_s, d2_r, o_s, o_r):
    chunk, width = xbuf.shape
    kv_heads = kv.shape[0] // 2
    heads = q.shape[0]
    group = heads // kv_heads
    n_blocks = seg.shape[0]
    quarter = wo.shape[0] // n_blocks
    pieces = y_s.shape[0]
    piece = quarter // pieces
    n_cols = width // COLS
    kv_tiles = 2 * kv_heads * HEAD // TILE
    q_tiles = heads * HEAD // TILE
    slots = wbuf.shape[0]

    dp = lax.axis_index('dp')
    tp = lax.axis_index('tp')
    me = lax.axis_index('cp')
    core_peer = me + 1 - 2 * lax.rem(me, 2)
    chip_peer = lax.rem(me + 2, 4)
    far_peer = 3 - me
    others = (core_peer, chip_peer, far_peer)
    tp_peer = (dp, 1 - tp, me)

    def at(block):
        return (dp, tp, block)

    def remote(src, dst, s_sem, r_sem, where):
        return pltpu.make_async_remote_copy(src_ref=src, dst_ref=dst, send_sem=s_sem, recv_sem=r_sem,
                                            device_id=where, device_id_type=MESH)

    odd = lax.rem(me, 2)
    barrier = pltpu.get_barrier_semaphore()
    pl.semaphore_signal(barrier, inc=1, device_id=tp_peer, device_id_type=MESH)

    @pl.when(odd == 0)
    def _():
        pl.semaphore_signal(barrier, inc=1, device_id=at(core_peer), device_id_type=MESH)

    @pl.when(odd == 1)
    def _():
        pl.semaphore_signal(barrier, inc=1, device_id=at(chip_peer), device_id_type=MESH)

    def kv_tile_src(t):
        per = kv_tiles // 2
        return (wk_hbm if t < per else wv_hbm).at[:, pl.ds((t % per) * TILE, TILE)]

    def tile_copy(src, slot):
        return pltpu.make_async_copy(src, wbuf.at[slot], tile_sem.at[slot])

    def q_tile_src(t):
        return wq_hbm.at[:, pl.ds(pl.multiple_of(t * TILE, TILE), TILE)]

    x_load = pltpu.make_async_copy(x_hbm, xbuf, load_sem.at[0])
    wo_load = pltpu.make_async_copy(wo_hbm, wo, load_sem.at[2])
    seg_load = pltpu.make_async_copy(seg_hbm, seg.at[me], load_sem.at[1])

    x_load.start()
    for t in range(kv_tiles):
        tile_copy(kv_tile_src(t), t).start()
    seg_load.start()


    def rows_of(block, i, moved):
        begin = -EXTRA if moved and i == 0 else 0
        end = -EXTRA if moved and i == pieces - 1 else 0
        return pl.ds(pl.multiple_of(block * quarter + i * piece + begin, 8), piece - begin + end)

    def by_piece(block, i, side, act):
        if 0 < i < pieces - 1:
            act(False)
            return
        low, high = EARLY if i == 0 else SHORT
        edge = (block >= low) & (block <= high) & (side == 0)
        for moved in (False, True):
            @pl.when(edge if moved else jnp.logical_not(edge))
            def _(moved=moved):
                act(moved)

    def y_copy(i, moved):
        rows = rows_of(me, i, moved)
        return remote(wo_hbm.at[rows], w_oth.at[rows], y_s.at[i], y_r.at[i], tp_peer)

    def hand_on(block, i, moved, s_sem, r_sem, where):
        part = w_oth.at[rows_of(block, i, moved)]
        return remote(part, part, s_sem.at[i], r_sem.at[i], where)

    def seg_copy(k, block, where):
        return remote(seg.at[block], seg.at[block], seg_s.at[k], seg_r.at[k], where)

    def kv_copy(k, block, where):
        part = kv.at[:, pl.ds(pl.multiple_of(block * chunk, chunk), chunk), :]
        return remote(part, part, kv_s.at[k], kv_r.at[k], where)

    def o_copy(k):
        part = pl.ds(*SENDS[k])
        return remote(o_own.at[part], o_oth.at[part], o_s.at[k], o_r.at[k], tp_peer)

    def group_of(j):
        high = lax.rem(me // 2 + j // 2, 2)
        low = lax.rem(lax.rem(me, 2) + lax.rem(j, 2), 2)
        return 2 * high + low

    def place_of(u):
        half = u // 6
        v = u - 6 * half
        end = v // 4
        j = (1 - half) * (v // 3) + half * (2 + (1 - end) * (v // 2) + end * (v - 4))
        i = (1 - half) * (v % 3) + half * ((1 - end) * (v % 2) + 2 * end)
        return j, i

    def head_of(u):
        j, i = place_of(u)
        return group_of(j) * group + i

    pl.semaphore_wait(barrier, 1 + 2 * odd)
    for i in range(pieces):
        by_piece(me, i, 1 - tp, lambda moved, i=i: y_copy(i, moved).start())

    @pl.when(odd == 1)
    def _():
        pl.semaphore_signal(entry, inc=1, device_id=at(chip_peer), device_id_type=MESH)
        pl.semaphore_wait(entry, 1)
        pl.semaphore_signal(entry, inc=1, device_id=at(core_peer), device_id_type=MESH)

    @pl.when(odd == 0)
    def _():
        pl.semaphore_wait(entry, 1)

    seg_load.wait()
    for k, block in enumerate(others):
        seg_copy(k, me, at(block)).start()

    x_load.wait()
    own_rows = pl.ds(pl.multiple_of(me * chunk, chunk), chunk)

    def project_kv(t, _):
        tile_copy(wk_hbm.at[:, pl.ds(0, TILE)], t).wait()
        part = jnp.dot(xbuf[...], wbuf[t], preferred_element_type=F32).astype(BF16)
        for k in range(TILE // HEAD):
            kv[t * (TILE // HEAD) + k, own_rows, :] = part[:, k * HEAD:(k + 1) * HEAD]

        @pl.when(t < q_tiles)
        def _():
            tile_copy(q_tile_src(t), t).start()
        return 0

    lax.fori_loop(0, kv_tiles, project_kv, 0)

    def project_q(t, _):
        slot = lax.rem(t, slots)
        tile_copy(q_tile_src(t), slot).wait()
        part = jnp.dot(xbuf[...], wbuf[slot], preferred_element_type=F32).astype(BF16)
        for k in range(TILE // HEAD):
            q[t * (TILE // HEAD) + k] = part[:, k * HEAD:(k + 1) * HEAD]

        @pl.when(t + slots < q_tiles)
        def _():
            tile_copy(q_tile_src(t + slots), slot).start()

        @pl.when(t == 0)
        def _():
            @pl.when(me < 2)
            def _():
                kv_copy(0, me, at(chip_peer)).start()
            kv_copy(1, me, at(core_peer)).start()
            wo_load.start()
        return 0

    lax.fori_loop(0, q_tiles, project_q, 0)

    def pass_y(i):
        def act(moved):
            y_copy(i, moved).wait_recv()
            hand_on(me, i, moved, xf_s, xf_r, at(chip_peer)).start()
            hand_on(me, i, moved, d1_s, d1_r, at(core_peer)).start()
        by_piece(me, i, tp, act)

    def pass_x(i):
        def act(moved):
            hand_on(chip_peer, i, moved, xf_s, xf_r, at(chip_peer)).wait_recv()
            hand_on(chip_peer, i, moved, d2_s, d2_r, at(core_peer)).start()
        by_piece(chip_peer, i, tp, act)

    def wait_near(i):
        by_piece(core_peer, i, tp, lambda moved: hand_on(core_peer, i, moved, d1_s, d1_r, at(core_peer)).wait_recv())

    def wait_far(i):
        by_piece(far_peer, i, tp, lambda moved: hand_on(far_peer, i, moved, d2_s, d2_r, at(core_peer)).wait_recv())

    pass_y(0)
    for k, block in enumerate(others):
        seg_copy(k, block, at(block)).wait_recv()
    seg_col = jnp.transpose(jnp.broadcast_to(seg[me], (HEAD, chunk)))
    segq[...] = seg_col

    kv_copy(1, core_peer, at(core_peer)).wait_recv()

    @pl.when(me >= 2)
    def _():
        kv_copy(0, chip_peer, at(chip_peer)).wait_recv()
        kv_copy(2, chip_peer, at(core_peer)).start()
        kv_copy(2, far_peer, at(core_peer)).wait_recv()

    def attend(u, h, g, r, n):
        rows = pl.ds(pl.multiple_of(r * TILE, TILE), TILE)
        q_t = q[h, rows, :]
        sq = segq[rows, :]
        sq = jnp.concatenate([sq] * (chunk // HEAD), axis=1)
        parts = []
        for b in range(n):
            s = lax.dot_general(q_t, kv[g, pl.ds(b * chunk, chunk), :], (((1,), (1,)), ((), ())), preferred_element_type=F32)
            ok = sq == seg[b]
            if b == n - 1:
                q_pos = r * TILE + lax.broadcasted_iota(jnp.int32, (TILE, chunk), 0)
                ok = ok & (q_pos >= lax.broadcasted_iota(jnp.int32, (TILE, chunk), 1))
            parts.append(jnp.where(ok, s, -jnp.inf))
        top = parts[0].max(axis=1, keepdims=True)
        for s in parts[1:]:
            top = jnp.maximum(top, s.max(axis=1, keepdims=True))
        total = None
        acc = None
        for b, s in enumerate(parts):
            p = jnp.exp2((s - top) * SCALE)
            row_sum = p.sum(axis=1, keepdims=True)
            pv = jnp.dot(p.astype(BF16), kv[kv_heads + g, pl.ds(b * chunk, chunk), :], preferred_element_type=F32)
            total = row_sum if total is None else total + row_sum
            acc = pv if acc is None else acc + pv
        o_own[u, rows, :] = (acc / total).astype(BF16)

    def attend_head(u, _):
        h = head_of(u)
        g = h // group
        for n in range(1, n_blocks + 1):
            @pl.when(me == n - 1)
            def _(n=n):
                def one(r, c):
                    attend(u, h, g, r, n)
                    return c
                lax.fori_loop(0, chunk // TILE, one, 0)

        for k, (begin, count) in enumerate(SENDS[:-1]):
            @pl.when(u == begin + count)
            def _(k=k):
                o_copy(k).start()

        @pl.when(u == group - 1)
        def _():
            pass_y(1)

        @pl.when(u == 3 * group - 1)
        def _():
            pass_x(0)
        return 0

    lax.fori_loop(0, heads, attend_head, 0)
    pass_y(2)

    def add_rows(o_ref, w_ref, y_ref, u, count, first):
        rows = pl.ds(pl.multiple_of(head_of(u) * HEAD, HEAD), count * HEAD)

        def one(c, carry):
            cols = pl.ds(pl.multiple_of(c * COLS, COLS), COLS)
            left = jnp.concatenate([o_ref[u + k] for k in range(count)], axis=1)
            part = jnp.dot(left, w_ref[rows, cols], preferred_element_type=F32)
            y_ref[:, cols] = part if first else y_ref[:, cols] + part
            return carry

        lax.fori_loop(0, n_cols, one, 0)

    wo_load.wait()
    runs = ((0, 3), (3, 3), (6, 2), (8, 2), (10, 1))
    for u, count in runs:
        add_rows(o_own, wo, y_own, u, count, u == 0)
        if u == 0:
            o_copy(len(SENDS) - 1).start()
    add_rows(o_own, wo, y_own, heads - 1, 1, False)

    pass_x(1)
    for u, count in runs:
        for k, (begin, _) in enumerate(SENDS):
            if u <= begin < u + count:
                o_copy(k).wait_recv()
        if u == 0:
            wait_near(0)
            wait_far(0)
        if u == 3:
            for i in range(1, pieces):
                wait_near(i)
        if u == 8:
            for i in range(1, pieces - 1):
                wait_far(i)
        if u == 10:
            pass_x(2)
        add_rows(o_oth, w_oth, y_oth, u, count, u == 0)
    wait_far(pieces - 1)

    o_copy(len(SENDS) - 1).wait_recv()

    for i in range(pieces):
        def sent(moved, i=i):
            hand_on(me, i, moved, xf_s, xf_r, at(chip_peer)).wait_send()
            hand_on(me, i, moved, d1_s, d1_r, at(core_peer)).wait_send()
        by_piece(me, i, 1 - tp, lambda moved, i=i: y_copy(i, moved).wait_send())
        by_piece(me, i, tp, sent)
        by_piece(chip_peer, i, tp, lambda moved, i=i: hand_on(chip_peer, i, moved, d2_s, d2_r, at(core_peer)).wait_send())
    for k, block in enumerate(others):
        seg_copy(k, me, at(block)).wait_send()
    kv_copy(1, me, at(core_peer)).wait_send()

    @pl.when(me < 2)
    def _():
        kv_copy(0, me, at(chip_peer)).wait_send()

    @pl.when(me >= 2)
    def _():
        kv_copy(2, chip_peer, at(core_peer)).wait_send()

    for k in range(len(SENDS)):
        o_copy(k).wait_send()


def last_kernel(last_head, y_own, y_oth, o_oth, w_oth, y_hbm, y_out, out_sem):
    h = last_head(lax.axis_index('cp'))
    left = o_oth[o_oth.shape[0] - 1]
    rows = pl.ds(pl.multiple_of(h * HEAD, HEAD), HEAD)
    copies = []
    for c in range(y_out.shape[1] // COLS):
        cols = pl.ds(c * COLS, COLS)
        part = jnp.dot(left, w_oth[rows, cols], preferred_element_type=F32)
        y_out[:, cols] = (y_own[:, cols] + (y_oth[:, cols] + part)).astype(BF16)
        copy = pltpu.make_async_copy(y_out.at[:, cols], y_hbm.at[:, cols], out_sem.at[c])
        copy.start()
        copies.append(copy)
    for copy in copies:
        copy.wait()


def solution(mesh):
    n_blocks = mesh.shape['cp']

    def layer(x_loc, seg_loc, w_query, w_key, w_value, w_out):
        chunk, width = x_loc.shape
        kv_heads = w_key.shape[1] // HEAD
        heads = w_query.shape[1] // HEAD
        pieces = 3
        dma = pltpu.SemaphoreType.DMA
        any_spec = pl.BlockSpec(memory_space=pl.ANY)
        vmem_spec = pl.BlockSpec(memory_space=pltpu.VMEM)
        parts = pl.pallas_call(
            layer_kernel,
            out_shape=(
                pltpu.VMEM((chunk, width), F32),
                pltpu.VMEM((chunk, width), F32),
                pltpu.VMEM((heads, chunk, HEAD), BF16),
                pltpu.VMEM(w_out.shape, BF16),
            ),
            in_specs=[any_spec] * 6,
            out_specs=[vmem_spec] * 4,
            scratch_shapes=[
                pltpu.VMEM((n_blocks, 1, chunk), jnp.int32),
                pltpu.VMEM((chunk, HEAD), jnp.int32),
                pltpu.VMEM((chunk, width), BF16),
                pltpu.VMEM((4, width, TILE), BF16),
                pltpu.VMEM((2 * kv_heads, n_blocks * chunk, HEAD), BF16),
                pltpu.VMEM((heads, chunk, HEAD), BF16),
                pltpu.VMEM((heads, chunk, HEAD), BF16),
                pltpu.VMEM(w_out.shape, BF16),
                pltpu.SemaphoreType.REGULAR, dma((3,)), dma((4,)),
                dma((3,)), dma((3,)), dma((3,)), dma((3,)),
                dma((pieces,)), dma((pieces,)), dma((pieces,)), dma((pieces,)),
                dma((pieces,)), dma((pieces,)), dma((pieces,)), dma((pieces,)),
                dma((len(SENDS),)), dma((len(SENDS),)),
            ],
            compiler_params=pltpu.CompilerParams(collective_id=0, has_side_effects=True, vmem_limit_bytes=36 * 2 ** 20),
        )(seg_loc.reshape(1, chunk), x_loc, w_query, w_key, w_value, w_out)
        parts = [pltpu.with_memory_space_constraint(a, pltpu.VMEM) for a in parts]

        def last_head(me):
            return (3 - me) * (heads // kv_heads) + heads // kv_heads - 1

        return pl.pallas_call(
            functools.partial(last_kernel, last_head),
            out_shape=jax.ShapeDtypeStruct((chunk, width), BF16),
            in_specs=[vmem_spec] * 4,
            out_specs=any_spec,
            scratch_shapes=[pltpu.VMEM((chunk, width), BF16), dma((width // COLS,))],
            compiler_params=pltpu.CompilerParams(vmem_limit_bytes=8 * 2 ** 20),
        )(*parts)

    rows = P(('dp', 'cp'), None)
    return jax.shard_map(layer, mesh=mesh,
                         in_specs=(rows, P(('dp', 'cp')), P(None, 'tp'), P(None, 'tp'), P(None, 'tp'), P('tp', None)),
                         out_specs=rows, check_vma=False)
```
